32 devices in a mesh: dp: 8 (over z, x), mp: 4 (over y, core).
Axes of the slice: x: 2, y: 2, z: 4, core: 2. Of those that a mesh axis runs over, the one named last changes fastest.
Arguments:
- sparse_vecs: bfloat16 [8192, 26, 128], P(('dp', 'mp')), may hold values from -6 to 6
- dense_vec: bfloat16 [8192, 128], P(('dp', 'mp')), may hold values from -6 to 6
- top_cot: bfloat16 [8192, 1024], P(('dp', 'mp')), may hold values from -0.59765625 to 0.59765625
- top_weight: bfloat16 [479, 1024], replicated, may hold values from -0.25 to 0.25
- owner_ids: int32 [8192, 26, 1], P(('dp', 'mp')), may hold values from 0 to 7; in each aligned block of 6656 rows (0 to 6655, 6656 to 13311, ..., all dimensions but the last counted through in order) at most 1664 rows name the same one
- local_rows: int32 [8192, 26], P(('dp', 'mp')), may hold values from 0 to 127
- table: float32 [26, 1024, 128], P(None, ('dp', 'mp')), may hold values from -0.6 to 0.6
- accum: float32 [26, 1024], P(None, ('dp', 'mp')), may hold values from 0.05 to 2
Outputs:
- dense_grad: bfloat16 [8192, 128], P(('dp', 'mp'))
- new_table: float32 [26, 1024, 128], P(None, ('dp', 'mp'))
- new_accum: float32 [26, 1024], P(None, ('dp', 'mp'))
The draws below stay inside these ranges and needn't reach their ends.
Inputs may be any that keep to these rules, and one draw needn't show every extreme that they name: `owner_ids`: among the lookups of one device's 256 samples no owner group is named more than 1664 times; in every draw some device names some owner group exactly 1664 times.
All inputs are finite; a program needn't handle non-finite values.
Results may differ from the reference program's by a relative error of at most 0.005.
Values may be sent and summed in bfloat16 or wider, within the bound.
A program may use at most 128 MiB of HBM per device.

```python
import math
import jax
import jax.numpy as jnp
import numpy as np
from jax import lax

E = 128
TABLES = 26
H1 = 1024
B_DEV = 256
ZIN = 479
BATCH = 8192
LOOK_DEV = 6656
ROWS_GRP = 128
ROWS = 1024
CAP = 1664
N_DP = 8


def with_ends(drawn, rng, low, high):
    place = [jax.random.randint(jax.random.fold_in(rng, axis), (), 0, length) for axis, length in enumerate(drawn.shape)]
    main_axis = drawn.shape.index(max(drawn.shape))
    next_to = place[:main_axis] + [(place[main_axis] + 1) % drawn.shape[main_axis]] + place[main_axis + 1:]
    return drawn.at[tuple(place)].set(low).at[tuple(next_to)].set(high)


def shard_levels(key, extent, pieces, low, largest):
    def one(axis_at, shards_of):
        steps = jax.random.uniform(jax.random.fold_in(jax.random.fold_in(key, 6), axis_at), (shards_of,), jnp.float32, low / len(pieces), largest / len(pieces))
        return jnp.repeat(jnp.exp(steps), extent[axis_at] // shards_of).reshape((-1,) + (1,) * (len(extent) - axis_at - 1))

    gain = one(*pieces[0])
    for cut in pieces[1:]:
        gain = gain * one(*cut)
    return gain


def rank_bounds(count, lean):
    loads = [(1 << 20) // math.isqrt(standing ** lean) + 1 for standing in range(1, count + 1)]
    spread = 1 + sum(loads) // (1 << 30)
    return np.cumsum(np.array([max(1, weight // spread) for weight in loads]))


def ranked(key, dims, amount, lean):
    listing = rank_bounds(amount, lean)
    ticket = jax.random.randint(jax.random.fold_in(key, 1), dims, 0, int(listing[amount - 1]))
    standing = jnp.searchsorted(jnp.asarray(listing, jnp.int32), ticket, side="right")
    return jax.random.permutation(jax.random.fold_in(key, 2), amount)[standing].astype(jnp.int32)


def shared_out(own_key, own, number, rows, number_of, top, most, slope):
    order = jax.random.permutation(own_key, number_of)
    heavy_load, usual = load_shares(number_of, rows * top, most, slope, True), load_shares(number_of, rows * top, most, slope, False)
    places = jnp.arange(number_of)

    def named(sizes, rotation):
        used = int((sizes > 0).sum())
        fixed = max(1, used // 4)
        moved = fixed + (places - fixed + rotation * (used - fixed)) % max(1, number_of - fixed)
        return jnp.zeros((number_of,), jnp.int32).at[order[jnp.where(places < fixed, places, moved)]].set(jnp.asarray(sizes, jnp.int32))

    sizes = jnp.where(number % 4 == 0, named(heavy_load, number // 4), named(usual, number - number // 4 - 1))
    mixed = jax.random.permutation(jax.random.fold_in(own, 3), number_of)
    donor, taker = mixed[0:number_of // 2 * 2:2], mixed[1:number_of // 2 * 2:2]
    room = jnp.minimum(sizes[donor] - 1, most - sizes[taker]) // 2
    room = jnp.where((donor == order[0]) | (taker == order[0]) | (sizes[taker] == 0), 0, jnp.maximum(room, 0))
    moved = jax.random.randint(jax.random.fold_in(own, 4), (number_of // 2,), 0, 1 << 20) % (room + 1)
    sizes = sizes.at[donor].add(-moved).at[taker].add(moved)
    members = jnp.searchsorted(jnp.cumsum(sizes), jnp.arange(rows * top), side="right").astype(jnp.int32)
    table = members.reshape(top, rows).T
    table = table[jax.random.permutation(jax.random.fold_in(own, 1), rows)]
    rotation = jax.random.randint(jax.random.fold_in(own, 2), (rows, 1), 0, top)
    return jnp.take_along_axis(table, (jnp.arange(top)[None, :] + rotation) % top, axis=1)


def load_shares(amount, total, most, lean, full):
    loads = [(1 << 20) // math.isqrt(grade ** lean) + 1 for grade in range(1, amount + 1)]
    largest = most if full else min(most, max(-(-total // amount), total * loads[0] // sum(loads)))
    least = 1 if total - largest >= amount - 1 else 0
    counts, surplus = [largest] + [least] * (amount - 1), total - largest - least * (amount - 1)
    while surplus > 0:
        free = [i for i in range(1, amount) if counts[i] < largest] or [i for i in range(1, amount) if counts[i] < most]
        pool, budget = sum([loads[i] for i in free]), surplus
        for i in free:
            more = min(most - counts[i], max(1, budget * loads[i] // pool), surplus)
            counts[i] = counts[i] + more
            surplus = surplus - more
    return np.array(counts)


def scatter_about(key, dims, scale, most, shards=(), kind=jnp.bfloat16):
    level = shard_levels(key, dims, shards, -0.22, 0.18) if shards else 1.0
    array = jax.random.normal(key, dims, jnp.float32) * scale * level
    return jnp.minimum(jnp.maximum(array, -most), most).astype(kind)


def setup_inputs(seed: int = 0) -> dict:
    seeds = jax.random.split(jax.random.key(seed), 9)
    sparse_vecs = scatter_about(seeds[0], (BATCH, TABLES, E), 1.0, 6.0, ((0, 32),))
    dense_vec = scatter_about(seeds[1], (BATCH, E), 1.0, 6.0, ((0, 32),))
    top_cot = scatter_about(seeds[2], (BATCH, H1), 0.1, 0.59765625, ((0, 32),))
    top_weight = scatter_about(seeds[3], (ZIN, H1), ZIN ** -0.5, 0.25)
    owner_ids_keys = jax.random.split(jax.random.fold_in(seeds[4], 1), BATCH * TABLES // LOOK_DEV)
    owner_ids_turns = jax.random.permutation(jax.random.fold_in(seeds[4], 3), BATCH * TABLES // LOOK_DEV)
    owner_ids = jax.vmap(lambda own, number: shared_out(jax.random.fold_in(seeds[4], 2), own, number, LOOK_DEV, N_DP, 1, CAP, 1))(owner_ids_keys, owner_ids_turns).reshape((BATCH, TABLES, 1))
    local_rows = with_ends(ranked(seeds[5], (BATCH, TABLES), ROWS_GRP, 2), jax.random.fold_in(seeds[5], 3), 0, ROWS_GRP - 1).astype(jnp.int32)
    table = scatter_about(seeds[6], (TABLES, ROWS, E), 0.1, 0.6, ((1, 32),), jnp.float32)
    accum = jnp.clip(jnp.exp(math.log(2.0) - 3.6888794 * jax.random.uniform(seeds[7], (TABLES, ROWS), jnp.float32) ** shard_levels(seeds[7], (TABLES, ROWS), ((1, 32),), -0.2, 0.2)), 0.05, 2.0)
    return dict(sparse_vecs=sparse_vecs, dense_vec=dense_vec, top_cot=top_cot, top_weight=top_weight, owner_ids=owner_ids, local_rows=local_rows, table=table, accum=accum)


LEARN_RATE = 0.1
EPSILON = 1e-08

def pair_matrix(feature_count):
    row_index, col_index = np.tril_indices(feature_count, -1)
    pair_count = row_index.shape[0]
    matrix = np.zeros((pair_count, feature_count * feature_count), np.float32)
    matrix[np.arange(pair_count), row_index * feature_count + col_index] = 1.0
    matrix[np.arange(pair_count), col_index * feature_count + row_index] = 1.0
    return matrix

def interaction(sparse_vecs, dense_vec, top_cot, top_weight):
    batch_rows, table_count, row_width = sparse_vecs.shape
    feature_count = table_count + 1
    input_cot = jnp.dot(top_cot, top_weight.T, preferred_element_type=jnp.float32)
    symmetric = jnp.dot(input_cot[:, row_width:], pair_matrix(feature_count), precision=lax.Precision.HIGHEST)
    symmetric = symmetric.reshape(batch_rows, feature_count, feature_count)
    features = jnp.concatenate([dense_vec[:, None, :], sparse_vecs], axis=1).astype(jnp.float32)
    feature_grad = jnp.einsum('bij,bje->bie', symmetric, features, precision=lax.Precision.HIGHEST)
    dense_grad = (input_cot[:, :row_width] + feature_grad[:, 0]).astype(jnp.bfloat16)
    sparse_grad = feature_grad[:, 1:].astype(jnp.bfloat16)
    return (dense_grad, sparse_grad)

def reference(sparse_vecs, dense_vec, top_cot, top_weight, owner_ids, local_rows, table, accum):
    block_count = BATCH // B_DEV

    def one_block(blocks):
        return interaction(blocks[0], blocks[1], blocks[2], top_weight)
    dense_grad, sparse_grad = lax.map(one_block, (sparse_vecs.reshape(block_count, B_DEV, TABLES, E), dense_vec.reshape(block_count, B_DEV, E), top_cot.reshape(block_count, B_DEV, H1)))
    dense_grad = dense_grad.reshape(BATCH, E)
    sparse_grad = sparse_grad.reshape(BATCH, TABLES, E)
    row_total = ROWS_GRP * N_DP
    row_keys = jnp.arange(TABLES, dtype=jnp.int32)[None, :] * row_total + owner_ids[:, :, 0] * ROWS_GRP + local_rows
    row_grad = jax.ops.segment_sum(sparse_grad.astype(jnp.float32).reshape(BATCH * TABLES, E), row_keys.reshape(BATCH * TABLES).astype(jnp.int32), num_segments=TABLES * row_total)
    row_grad = row_grad.reshape(TABLES, row_total, E)
    new_accum = accum + lax.optimization_barrier(jnp.mean(row_grad * row_grad, axis=-1))
    new_table = table - LEARN_RATE * row_grad / (jnp.sqrt(new_accum)[:, :, None] + EPSILON)
    return (dense_grad, new_table, new_accum)
```

```python
import functools

import jax
import jax.numpy as jnp
from jax import lax
from jax.experimental import pallas as pl
from jax.experimental.pallas import tpu as pltpu
from jax.sharding import PartitionSpec as P

LEARN_RATE = 0.1
EPSILON = 1e-08
MESH = pl.DeviceIdType.MESH
VMEM_LIMIT = 60 * 1024 * 1024
LANES = 128
GROUP = 8
SPAN = 256


def table_slots(table_count, handlers, half):
    slots = []
    for start in range(0, table_count, handlers):
        count = min(handlers, table_count - start)
        if count == handlers:
            slots.append((start, None))
        else:
            step = handlers // count
            owners = [(i * step + (i % 2) * half) % handlers for i in range(count)]
            if len(set(owners)) < count:
                owners = list(range(count))
            slots.append((start, tuple(owners)))
    return slots


def step_kernel(
    slots, z_count, mp_count,
    sparse, dense, cot, weight, owner, local, table, accum,
    dense_out, table_out, accum_out,
    feats, cot_v, weight_v, owner_v, local_v, table_v, accum_v,
    keys, blocks, spread, top, grads, got_rows, got_keys,
    partial, own_sum, z_in, fin_out, fin_in, turned,
    load_sem, self_sem, key_send, key_recv, row_send, row_recv,
    z_send, z_recv, fin_send, fin_recv,
):
    table_count, batch_rows, width = sparse.shape
    rows_own = table.shape[1]
    handlers = 2 * mp_count
    rows_grp = rows_own * mp_count
    block = handlers * rows_own
    feature_count = table_count + 1
    dp, mp = lax.axis_index("dp"), lax.axis_index("mp")
    z, x = dp // 2, dp % 2
    me = x * mp_count + mp

    def plane_device(h):
        return (z * 2 + h // mp_count, h % mp_count)

    def z_device(d):
        return (((z + d) % z_count) * 2 + x, mp)

    loads = [
        pltpu.make_async_copy(source, target, load_sem.at[i])
        for i, (source, target) in enumerate((
            (cot, cot_v), (weight, weight_v), (owner, owner_v), (local, local_v),
            (sparse, feats.at[pl.ds(0, table_count)]), (dense, feats.at[table_count]),
            (table, table_v), (accum, accum_v),
        ))
    ]
    for load in loads:
        load.start()

    peers = [plane_device((me + d) % handlers) for d in range(1, handlers)]
    peers_z = [z_device(d) for d in range(1, z_count)]
    barrier = pltpu.get_barrier_semaphore()
    for device in peers + peers_z:
        pl.semaphore_signal(barrier, inc=1, device_id=device, device_id_type=MESH)

    started = []

    def begin(copy):
        copy.start()
        started.append(copy)
        return copy

    loads[0].wait()
    loads[1].wait()
    input_cot = lax.dot_general(
        cot_v[...], weight_v[...], (((1,), (1,)), ((), ())), preferred_element_type=jnp.float32
    )
    top[...] = input_cot[:, :width]
    pair_count = feature_count * (feature_count - 1) // 2
    feature_pad = SPAN // GROUP
    per_dot = LANES // feature_pad
    dots = -(-feature_count // per_dot)
    columns = lax.broadcasted_iota(jnp.int32, (1, dots * LANES), 1)
    left, right = columns // feature_pad, columns % feature_pad
    inside = (left < feature_count) & (right < feature_count) & (left != right)
    left = jnp.where(left == table_count, 0, left + 1)
    right = jnp.where(right == table_count, 0, right + 1)
    high, low = jnp.maximum(left, right), jnp.minimum(left, right)
    place = jnp.where(inside, high * (high - 1) // 2 + low, -1)
    pairs = lax.broadcasted_iota(jnp.int32, (pair_count, dots * LANES), 0)
    select = jnp.where(pairs == place, 1.0, 0.0).astype(jnp.bfloat16)
    symmetric = jnp.dot(
        input_cot[:, width:].astype(jnp.bfloat16), select, preferred_element_type=jnp.float32
    ).astype(jnp.bfloat16)
    rep_row = lax.broadcasted_iota(jnp.int32, (LANES, per_dot * SPAN), 0)
    rep_col = lax.broadcasted_iota(jnp.int32, (LANES, per_dot * SPAN), 1)
    repeat = jnp.where(rep_row == rep_col // GROUP, 1.0, 0.0).astype(jnp.bfloat16)

    loads[2].wait()
    loads[3].wait()
    for t in range(table_count):
        keys[t] = owner_v[t] * rows_grp + local_v[t : t + 1]

    loads[4].wait()
    loads[5].wait()

    def build_blocks(i, carry):
        span = pl.ds(pl.multiple_of(i * 2 * GROUP, 2 * GROUP), 2 * GROUP)
        both = feats[:, span, :].astype(jnp.float32)
        pad = jnp.zeros(((feature_pad - feature_count) * GROUP, width), jnp.float32)
        for half in range(2):
            part = both[:, half * GROUP : (half + 1) * GROUP, :]
            part = part.reshape(feature_count * GROUP, width)
            blocks[2 * i + half] = jnp.concatenate([part, pad], 0).astype(jnp.bfloat16)
        return carry

    lax.fori_loop(0, batch_rows // (2 * GROUP), build_blocks, 0)

    mask = (
        lax.broadcasted_iota(jnp.int32, (GROUP, SPAN), 1) % GROUP
        == lax.broadcasted_iota(jnp.int32, (GROUP, SPAN), 0)
    )

    def gradients(first, last):
        for q in range(first // per_dot, -(-last // per_dot)):
            spread[:, q * per_dot * SPAN : (q + 1) * per_dot * SPAN] = jnp.dot(
                symmetric[:, q * LANES : (q + 1) * LANES], repeat,
                preferred_element_type=jnp.float32,
            )

        def one(i, carry):
            outs = []
            for half in range(2):
                rows = pl.ds(pl.multiple_of((2 * i + half) * GROUP, GROUP), GROUP)
                parts = [
                    jnp.where(mask, spread[rows, t * SPAN : (t + 1) * SPAN], 0.0)
                    for t in range(first, last)
                ]
                lhs = jnp.concatenate(parts, 0).astype(jnp.bfloat16)
                outs.append(
                    jnp.dot(lhs, blocks[2 * i + half], preferred_element_type=jnp.float32)
                )
            span = pl.ds(pl.multiple_of(i * 2 * GROUP, 2 * GROUP), 2 * GROUP)
            for t in range(first, last):
                at = (t - first) * GROUP
                both = jnp.concatenate([out[at : at + GROUP] for out in outs], 0)
                if t == table_count:
                    dense_out[span, :] = (both + top[span, :]).astype(jnp.bfloat16)
                else:
                    grads[t, span, :] = both.astype(jnp.bfloat16)
            return carry

        lax.fori_loop(0, batch_rows // (2 * GROUP), one, 0)

    def row_copy(slot, t, d):
        return pltpu.make_async_remote_copy(
            src_ref=grads.at[t],
            dst_ref=got_rows.at[slot, me],
            send_sem=row_send.at[slot, d - 1],
            recv_sem=row_recv.at[slot, d - 1],
            device_id=plane_device((me + d) % handlers),
            device_id_type=MESH,
        )

    def key_copy(slot, t, d):
        return pltpu.make_async_remote_copy(
            src_ref=keys.at[t],
            dst_ref=got_keys.at[slot, me],
            send_sem=key_send.at[slot, d - 1],
            recv_sem=key_recv.at[slot, d - 1],
            device_id=plane_device((me + d) % handlers),
            device_id_type=MESH,
        )

    def self_copies(slot, t):
        return [
            pltpu.make_async_copy(grads.at[t], got_rows.at[slot, me], self_sem.at[slot, 0]),
            pltpu.make_async_copy(keys.at[t], got_keys.at[slot, me], self_sem.at[slot, 1]),
        ]

    def each_send(slot, action, kind):
        start, owners = slots[slot]
        make = row_copy if kind == "rows" else key_copy
        for d in range(1, handlers):
            target = (me + d) % handlers
            if owners is None:
                action(make(slot, start + target, d))
            else:
                for i, h in enumerate(owners):
                    @pl.when(target == h)
                    def _(i=i):
                        action(make(slot, start + i, d))

    def handled(slot, body):
        start, owners = slots[slot]
        if owners is None:
            body(start + me)
        else:
            for i, h in enumerate(owners):
                @pl.when(me == h)
                def _(i=i):
                    body(start + i)

    def send_slot(slot):
        each_send(slot, lambda copy: copy.start(), "keys")
        each_send(slot, lambda copy: copy.start(), "rows")

        def own(t):
            for copy in self_copies(slot, t):
                copy.start()

        handled(slot, own)

    def z_copy(slot, d):
        return pltpu.make_async_remote_copy(
            src_ref=partial.at[slot, d - 1],
            dst_ref=z_in.at[slot, d - 1],
            send_sem=z_send.at[slot, d - 1],
            recv_sem=z_recv.at[slot, d - 1],
            device_id=z_device(d),
            device_id_type=MESH,
        )

    lookups = handlers * batch_rows

    def job(slot):
        def body(t):
            for copy in self_copies(slot, t):
                copy.wait()
            for d in range(1, handlers):
                row_copy(slot, t, d).wait_recv()
                key_copy(slot, t, d).wait_recv()
            targets = lax.broadcasted_iota(jnp.int32, (block, batch_rows), 0)

            def sums(d):
                base = ((z + d) % z_count) * block
                total = jnp.zeros((block, width), jnp.float32)
                for h in range(handlers):
                    onehot = jnp.where(targets == got_keys[slot, h] - base, 1.0, 0.0)
                    total = total + jnp.dot(
                        onehot.astype(jnp.bfloat16), got_rows[slot, h],
                        preferred_element_type=jnp.float32,
                    )
                return total

            def away(step, carry):
                d = step + 1
                partial[slot, step] = sums(d).astype(jnp.bfloat16)
                z_copy(slot, d).start()
                return carry

            lax.fori_loop(0, z_count - 1, away, 0)
            own_sum[slot] = sums(0)

        handled(slot, body)

    def fin_copy(slot, t, d):
        target = (me + d) % handlers
        return pltpu.make_async_remote_copy(
            src_ref=fin_out.at[slot, target],
            dst_ref=fin_in.at[t],
            send_sem=fin_send.at[slot, d - 1],
            recv_sem=fin_recv.at[slot, d - 1],
            device_id=plane_device(target),
            device_id_type=MESH,
        )

    def finish(slot):
        def body(t):
            def wait(step, carry):
                z_copy(slot, step + 1).wait_recv()
                return carry

            lax.fori_loop(0, z_count - 1, wait, 0)
            total = own_sum[slot]
            for d in range(1, z_count):
                total = total + z_in[slot, d - 1].astype(jnp.float32)
            total = total.astype(jnp.bfloat16)
            for h in range(handlers):
                fin_out[slot, h] = total[h * rows_own : (h + 1) * rows_own]
            for d in range(1, handlers):
                fin_copy(slot, t, d).start()
            fin_in[t] = fin_out[slot, me]

        handled(slot, body)

    lane = lax.broadcasted_iota(jnp.int32, (rows_own, LANES), 1)
    state = {}

    def update(slot):
        start, owners = slots[slot]
        count = handlers if owners is None else len(owners)
        for d in range(1, handlers):
            source = (me - d + handlers) % handlers
            if owners is None:
                fin_copy(slot, start, d).wait_recv()
            else:
                for i, h in enumerate(owners):
                    @pl.when(source == h)
                    def _():
                        fin_copy(slot, start, d).wait_recv()
        for t in range(start, start + count):
            grad = fin_in[t].astype(jnp.float32)
            mean = jnp.sum(grad * grad, axis=1, keepdims=True) * (1.0 / width)
            new = state["old"][:, t : t + 1] + mean
            state["new"] = jnp.where(lane == t, new, state["new"])
            table_out[t] = table_v[t] - LEARN_RATE * grad / (jnp.sqrt(new) + EPSILON)

    def rows_of(slot):
        start, owners = slots[slot]
        return start, start + (handlers if owners is None else len(owners))

    count = len(slots)
    for slot in range(count):
        first, last = rows_of(slot)
        gradients(first, last + (1 if slot == count - 1 else 0))
        if slot == 0:
            pl.semaphore_wait(barrier, handlers - 1 + z_count - 1)
        send_slot(slot)

    loads[6].wait()
    loads[7].wait()
    old = jnp.concatenate(
        [accum_v[...], jnp.zeros((LANES - table_count, rows_own), jnp.float32)], 0
    )
    state["old"] = old.T
    state["new"] = jnp.zeros((rows_own, LANES), jnp.float32)

    for step in range(count + 2):
        if step < count:
            job(step)
        if 0 <= step - 1 < count:
            finish(step - 1)
        if 0 <= step - 2 < count:
            update(step - 2)
    accum_out[...] = state["new"].T[:table_count]

    for slot in range(count):
        each_send(slot, lambda copy: copy.wait_send(), "rows")
        each_send(slot, lambda copy: copy.wait_send(), "keys")

        def sent(t):
            def wait(step, carry):
                z_copy(slot, step + 1).wait_send()
                return carry

            lax.fori_loop(0, z_count - 1, wait, 0)
            for d in range(1, handlers):
                fin_copy(slot, t, d).wait_send()

        handled(slot, sent)


def per_device(sparse_vecs, dense_vec, top_cot, top_weight, owner_ids, local_rows, table, accum):
    batch_rows, table_count, width = sparse_vecs.shape
    rows_own = table.shape[1]
    z_count = lax.axis_size("dp") // 2
    mp_count = lax.axis_size("mp")
    handlers = 2 * mp_count
    slots = table_slots(table_count, handlers, mp_count // 2)
    count = len(slots)
    block = handlers * rows_own
    feature_count = table_count + 1
    dots = -(-feature_count * (SPAN // GROUP) // LANES)
    others = max(1, z_count - 1)
    near = handlers - 1
    any_spec = pl.BlockSpec(memory_space=pl.ANY)
    vmem = pl.BlockSpec(memory_space=pltpu.VMEM)
    dma = pltpu.SemaphoreType.DMA
    bf16, f32, i32 = jnp.bfloat16, jnp.float32, jnp.int32
    out_shape = (
        jax.ShapeDtypeStruct(dense_vec.shape, bf16),
        jax.ShapeDtypeStruct(table.shape, f32),
        jax.ShapeDtypeStruct(accum.shape, f32),
    )
    scratch = [
        pltpu.VMEM((feature_count, batch_rows, width), bf16),
        pltpu.VMEM(top_cot.shape, bf16),
        pltpu.VMEM(top_weight.shape, bf16),
        pltpu.VMEM((table_count, 1, batch_rows), i32),
        pltpu.VMEM((table_count, batch_rows), i32),
        pltpu.VMEM(table.shape, f32),
        pltpu.VMEM(accum.shape, f32),
        pltpu.VMEM((table_count, 1, batch_rows), i32),
        pltpu.VMEM((batch_rows // GROUP, SPAN, width), bf16),
        pltpu.VMEM((batch_rows, dots * (LANES // (SPAN // GROUP)) * SPAN), f32),
        pltpu.VMEM((batch_rows, width), f32),
        pltpu.VMEM((table_count, batch_rows, width), bf16),
        pltpu.VMEM((count, handlers, batch_rows, width), bf16),
        pltpu.VMEM((count, handlers, 1, batch_rows), i32),
        pltpu.VMEM((count, others, block, width), bf16),
        pltpu.VMEM((count, block, width), f32),
        pltpu.VMEM((count, others, block, width), bf16),
        pltpu.VMEM((count, handlers, rows_own, width), bf16),
        pltpu.VMEM((table_count, rows_own, width), bf16),
        pltpu.VMEM((rows_own, LANES), f32),
        dma((8,)),
        dma((count, 2)),
        dma((count, near)),
        dma((count, near)),
        dma((count, near)),
        dma((count, near)),
        dma((count, others)),
        dma((count, others)),
        dma((count, near)),
        dma((count, near)),
    ]
    return pl.pallas_call(
        functools.partial(step_kernel, slots, z_count, mp_count),
        out_shape=out_shape,
        in_specs=[any_spec] * 8,
        out_specs=(vmem,) * 3,
        scratch_shapes=scratch,
        compiler_params=pltpu.CompilerParams(
            collective_id=0, has_side_effects=True, vmem_limit_bytes=VMEM_LIMIT
        ),
    )(
        sparse_vecs.transpose(1, 0, 2), dense_vec, top_cot, top_weight,
        owner_ids.transpose(1, 2, 0), local_rows.T, table, accum,
    )


def solution(mesh):
    in_specs = (
        P(("dp", "mp"), None, None),
        P(("dp", "mp"), None),
        P(("dp", "mp"), None),
        P(),
        P(("dp", "mp"), None, None),
        P(("dp", "mp"), None),
        P(None, ("dp", "mp"), None),
        P(None, ("dp", "mp")),
    )
    out_specs = (P(("dp", "mp"), None), P(None, ("dp", "mp"), None), P(None, ("dp", "mp")))
    return jax.shard_map(
        per_device, mesh=mesh, in_specs=in_specs, out_specs=out_specs, check_vma=False
    )
```

```python
import functools

import jax
import jax.numpy as jnp
from jax import lax
from jax.experimental import pallas as pl
from jax.experimental.pallas import tpu as pltpu
from jax.sharding import PartitionSpec as P

LEARN_RATE = 0.1
EPSILON = 1e-08
MESH = pl.DeviceIdType.MESH
VMEM_LIMIT = 60 * 1024 * 1024
LANES = 128
GROUP = 8
SPAN = 256
UNROLL = 4
PARTS = (2, 14, 26)


def table_slots(table_count, handlers):
    slots = []
    rest = table_count % handlers
    starts = [0] * (rest > 0) + list(range(rest, table_count, handlers))
    for start in starts:
        count = rest if rest and start == 0 else handlers
        if count == handlers:
            slots.append((start, None))
        else:
            step = 2 if 2 * count <= handlers else 1
            owners = [handlers - step * (count - i) for i in range(count)]
            slots.append((start, tuple(owners)))
    return slots


def step_kernel(
    slots, z_count, mp_count,
    sparse, dense, cot, weight, owner, local, table, accum,
    dense_out, table_out, accum_out,
    feats, cot_v, weight_v, owner_v, local_v, table_v, accum_v,
    keys, select, repeat, blocks, spread, top, grads, got_rows, got_keys,
    partial, own_sum, z_in, fin_out, fin_in,
    load_sem, self_sem, key_send, key_recv, row_send, row_recv,
    z_send, z_recv, fin_send, fin_recv,
):
    table_count, batch_rows, width = sparse.shape
    rows_own = table.shape[1]
    handlers = 2 * mp_count
    rows_grp = rows_own * mp_count
    block = handlers * rows_own
    feature_count = table_count + 1
    dp, mp = lax.axis_index("dp"), lax.axis_index("mp")
    z, x = dp // 2, dp % 2
    me = x * mp_count + mp

    def plane_device(h):
        return (z * 2 + h // mp_count, h % mp_count)

    def z_device(d):
        return (((z + d) % z_count) * 2 + x, mp)

    loads = [
        pltpu.make_async_copy(source, target, load_sem.at[i])
        for i, (source, target) in enumerate((
            (cot, cot_v), (weight, weight_v), (owner, owner_v), (local, local_v),
            (sparse, feats.at[pl.ds(0, table_count)]), (dense, feats.at[table_count]),
            (table, table_v), (accum, accum_v),
        ))
    ]
    for load in loads:
        load.start()

    peers = [plane_device((me + d) % handlers) for d in range(1, handlers)]
    peers_z = [z_device(d) for d in range(1, z_count)]
    barrier = pltpu.get_barrier_semaphore()
    for device in peers + peers_z:
        pl.semaphore_signal(barrier, inc=1, device_id=device, device_id_type=MESH)

    with jax.named_scope("const"):
        pair_count = feature_count * (feature_count - 1) // 2
        feature_pad = SPAN // GROUP
        per_dot = LANES // feature_pad
        dots = -(-feature_count // per_dot)
        columns = lax.broadcasted_iota(jnp.int32, (1, dots * LANES), 1)
        left, right = columns // feature_pad, columns % feature_pad
        inside = (left < feature_count) & (right < feature_count) & (left != right)
        left = jnp.where(left == table_count, 0, left + 1)
        right = jnp.where(right == table_count, 0, right + 1)
        high, low = jnp.maximum(left, right), jnp.minimum(left, right)
        place = jnp.where(inside, high * (high - 1) // 2 + low, -1)
        pairs = lax.broadcasted_iota(jnp.int32, (pair_count, dots * LANES), 0)
        select[...] = jnp.where(pairs == place, 1.0, 0.0).astype(jnp.bfloat16)
        rep_row = lax.broadcasted_iota(jnp.int32, (LANES, per_dot * SPAN), 0)
        rep_col = lax.broadcasted_iota(jnp.int32, (LANES, per_dot * SPAN), 1)
        repeat[...] = jnp.where(rep_row == rep_col // GROUP, 1.0, 0.0).astype(jnp.bfloat16)
    with jax.named_scope("loadwait"):
        loads[0].wait()
        loads[1].wait()
    input_cot = lax.dot_general(
        cot_v[...], weight_v[...], (((1,), (1,)), ((), ())), preferred_element_type=jnp.float32
    )
    top[...] = input_cot[:, :width]
    symmetric = jnp.dot(
        input_cot[:, width:].astype(jnp.bfloat16), select[...], preferred_element_type=jnp.float32
    ).astype(jnp.bfloat16)

    loads[4].wait()
    loads[5].wait()

    def build_blocks(i, carry):
        span = pl.ds(pl.multiple_of(i * 2 * GROUP, 2 * GROUP), 2 * GROUP)
        both = feats[:, span, :].astype(jnp.float32)
        pad = jnp.zeros(((feature_pad - feature_count) * GROUP, width), jnp.float32)
        for half in range(2):
            part = both[:, half * GROUP : (half + 1) * GROUP, :]
            part = part.reshape(feature_count * GROUP, width)
            blocks[2 * i + half] = jnp.concatenate([part, pad], 0).astype(jnp.bfloat16)
        return carry

    with jax.named_scope("blocks"):
        lax.fori_loop(0, batch_rows // (2 * GROUP), build_blocks, 0)

    mask = (
        lax.broadcasted_iota(jnp.int32, (GROUP, SPAN), 1) % GROUP
        == lax.broadcasted_iota(jnp.int32, (GROUP, SPAN), 0)
    )

    def gradients(first, last):
        for q in range(first // per_dot, -(-last // per_dot)):
            spread[:, q * per_dot * SPAN : (q + 1) * per_dot * SPAN] = jnp.dot(
                symmetric[:, q * LANES : (q + 1) * LANES], repeat[...],
                preferred_element_type=jnp.float32,
            )

        def one(step, carry):
            for i in [step * UNROLL + u for u in range(UNROLL)]:
                outs = []
                for half in range(2):
                    rows = pl.ds(pl.multiple_of((2 * i + half) * GROUP, GROUP), GROUP)
                    parts = [
                        jnp.where(mask, spread[rows, t * SPAN : (t + 1) * SPAN], 0.0)
                        for t in range(first, last)
                    ]
                    lhs = jnp.concatenate(parts, 0).astype(jnp.bfloat16)
                    outs.append(
                        jnp.dot(lhs, blocks[2 * i + half], preferred_element_type=jnp.float32)
                    )
                span = pl.ds(pl.multiple_of(i * 2 * GROUP, 2 * GROUP), 2 * GROUP)
                for t in range(first, last):
                    at = (t - first) * GROUP
                    both = jnp.concatenate([out[at : at + GROUP] for out in outs], 0)
                    if t == table_count:
                        dense_out[span, :] = (both + top[span, :]).astype(jnp.bfloat16)
                    else:
                        grads[t, span, :] = both.astype(jnp.bfloat16)
            return carry

        lax.fori_loop(0, batch_rows // (2 * GROUP * UNROLL), one, 0)

    def table_of(slot, h):
        return slots[slot][0] + h // 2 + (h % 2) * (handlers // 2)

    def row_copy(slot, t, target, source):
        return pltpu.make_async_remote_copy(
            src_ref=grads.at[t],
            dst_ref=got_rows.at[slot, source],
            send_sem=row_send.at[slot, target],
            recv_sem=row_recv.at[slot, source],
            device_id=plane_device(target),
            device_id_type=MESH,
        )

    def key_copy(target, source):
        return pltpu.make_async_remote_copy(
            src_ref=keys.at[target],
            dst_ref=got_keys.at[source],
            send_sem=key_send.at[target],
            recv_sem=key_recv.at[source],
            device_id=plane_device(target),
            device_id_type=MESH,
        )

    def self_copy(slot, t):
        return pltpu.make_async_copy(grads.at[t], got_rows.at[slot, me], self_sem.at[slot])

    def targets_of(slot, parity):
        start, owners = slots[slot]
        if owners is None:
            for j in range(1, handlers // 2):
                h = 2 * ((me // 2 + j) % (handlers // 2)) + parity
                yield h, table_of(slot, h), None
            h = 2 * (me // 2) + parity
            yield h, table_of(slot, h), me != h
        else:
            for i, h in enumerate(owners):
                if h % 2 == parity:
                    yield h, start + i, me != h

    def guarded(condition, body):
        if condition is None:
            body()
        else:
            pl.when(condition)(body)

    def handled(slot, body, parity=None):
        start, owners = slots[slot]
        if owners is None:
            if parity is None:
                body(table_of(slot, me))
            else:
                guarded(me % 2 == parity, lambda: body(table_of(slot, me)))
        else:
            for i, h in enumerate(owners):
                if parity is None or h % 2 == parity:
                    guarded(me == h, lambda i=i: body(start + i))

    def send_rows(slot, parity):
        for h, t, condition in targets_of(slot, parity):
            guarded(condition, lambda: row_copy(slot, t, h, me).start())
        handled(slot, lambda t: self_copy(slot, t).start(), parity)

    def build_keys():
        for slot, (start, owners) in enumerate(slots):
            for h in range(handlers):
                if owners is None:
                    t = table_of(slot, h)
                else:
                    t = start + (owners.index(h) if h in owners else 0)
                keys[h, slot] = owner_v[t] * rows_grp + local_v[t : t + 1]
        for slot in range(len(slots)):
            got_keys[me, slot] = keys[me, slot]

    def send_keys():
        for d in range(1, handlers):
            key_copy((me + d) % handlers, me).start()

    def wait_sent(slot):
        for parity in range(2):
            for h, t, condition in targets_of(slot, parity):
                guarded(condition, lambda: row_copy(slot, t, h, me).wait_send())

    def z_order(step):
        low = z_count - 1 - step
        low = low - jnp.where(low <= z, 1, 0)
        high = step + jnp.where(step >= z, 1, 0)
        return jnp.where(2 * z < z_count, low, high)

    def z_copy(slot, target, source):
        return pltpu.make_async_remote_copy(
            src_ref=partial.at[slot, target],
            dst_ref=z_in.at[slot, source],
            send_sem=z_send.at[slot, target],
            recv_sem=z_recv.at[slot, source],
            device_id=(target * 2 + x, mp),
            device_id_type=MESH,
        )

    def job(slot):
        def body(t):
            with jax.named_scope(f"jobwait{slot}"):
                self_copy(slot, t).wait()
                for d in range(1, handlers):
                    source = (me + d) % handlers
                    row_copy(slot, t, source, source).wait_recv()
            targets = lax.broadcasted_iota(jnp.int32, (block, batch_rows), 0)

            def sums(target):
                base = target * block
                total = jnp.zeros((block, width), jnp.float32)
                for h in range(handlers):
                    onehot = jnp.where(targets == got_keys[h, slot] - base, 1.0, 0.0)
                    total = total + jnp.dot(
                        onehot.astype(jnp.bfloat16), got_rows[slot, h],
                        preferred_element_type=jnp.float32,
                    )
                return total

            def away(step, carry):
                target = z_order(step)
                partial[slot, target] = sums(target).astype(jnp.bfloat16)
                z_copy(slot, target, z).start()
                return carry

            lax.fori_loop(0, z_count - 1, away, 0)
            own_sum[slot] = sums(z)

        handled(slot, body)

    def fin_copy(slot, t, target, source):
        return pltpu.make_async_remote_copy(
            src_ref=fin_out.at[slot, target],
            dst_ref=fin_in.at[t],
            send_sem=fin_send.at[slot, target],
            recv_sem=fin_recv.at[slot, source],
            device_id=plane_device(target),
            device_id_type=MESH,
        )

    def finish(slot):
        def body(t):
            def wait(step, carry):
                source = (z + 1 + step) % z_count
                z_copy(slot, source, source).wait_recv()
                return carry

            with jax.named_scope(f"finwait{slot}"):
                lax.fori_loop(0, z_count - 1, wait, 0)
            total = own_sum[slot]
            for d in range(1, z_count):
                total = total + z_in[slot, (z + d) % z_count].astype(jnp.float32)
            total = total.astype(jnp.bfloat16)
            for h in range(handlers):
                fin_out[slot, h] = total[h * rows_own : (h + 1) * rows_own]
            for d in range(1, handlers):
                fin_copy(slot, t, (me + d) % handlers, me).start()
            fin_in[t] = fin_out[slot, me]

        handled(slot, body)

    lane = lax.broadcasted_iota(jnp.int32, (rows_own, LANES), 1)
    state = {}

    def update(slot):
        start, owners = slots[slot]
        count = handlers if owners is None else len(owners)
        if owners is None:
            for d in range(1, handlers):
                source = (me + d) % handlers
                fin_copy(slot, table_of(slot, source), source, source).wait_recv()
        else:
            for i, h in enumerate(owners):
                guarded(me != h, lambda: fin_copy(slot, start + i, h, h).wait_recv())
        span = slice(start, start + count)
        grad = fin_in[span].astype(jnp.float32)
        mean = jnp.sum(grad * grad, axis=2, keepdims=True) * (1.0 / width)
        old = jnp.stack([state["old"][:, t : t + 1] for t in range(start, start + count)])
        new = old + mean
        for i in range(count):
            state["new"] = jnp.where(lane == start + i, new[i], state["new"])
        table_out[span] = table_v[span] - grad * (LEARN_RATE / (jnp.sqrt(new) + EPSILON))

    def rows_of(slot):
        start, owners = slots[slot]
        return start, start + (handlers if owners is None else len(owners))

    count = len(slots)
    sends = []
    for slot in range(count):
        first, last = rows_of(slot)
        if slots[slot][1] is None:
            sends += [(slot, 0, first + handlers // 2), (slot, 1, last)]
        else:
            sends += [(slot, 0, last), (slot, 1, last)]
    done = 0
    for part, last in enumerate(PARTS):
        last = min(last, table_count)
        if part == len(PARTS) - 1:
            last = table_count
        with jax.named_scope(f"grad{part}"):
            gradients(done, last + (1 if last == table_count else 0))
        if part == 0:
            loads[2].wait()
            loads[3].wait()
            build_keys()
            with jax.named_scope("barrier"):
                pl.semaphore_wait(barrier, handlers - 1 + z_count - 1)
            send_keys()
        for slot, parity, ready in sends:
            if done < ready <= last or (parity and ready == last == table_count):
                send_rows(slot, parity)
        done = last

    loads[6].wait()
    loads[7].wait()
    old = jnp.concatenate(
        [accum_v[...], jnp.zeros((LANES - table_count, rows_own), jnp.float32)], 0
    )
    state["old"] = old.T
    state["new"] = jnp.zeros((rows_own, LANES), jnp.float32)

    for d in range(1, handlers):
        source = (me + d) % handlers
        key_copy(source, source).wait_recv()

    plan = []
    for step in range(count + 1):
        plan += [(job, step)] * (step < count) + [(finish, step - 1)] * (step > 0)
    last = plan.pop()
    plan += [(update, slot) for slot in range(count - 2)] + [last]
    plan += [(update, slot) for slot in range(max(0, count - 2), count)]
    for stage, slot in plan:
        with jax.named_scope(f"{stage.__name__}{slot}"):
            stage(slot)
    with jax.named_scope("accum"):
        accum_out[...] = state["new"].T[:table_count]

    for d in range(1, handlers):
        key_copy((me + d) % handlers, me).wait_send()
    for slot in range(count):
      with jax.named_scope("sent"):
        wait_sent(slot)

        def sent(t):
            def wait(step, carry):
                target = (z + 1 + step) % z_count
                z_copy(slot, target, z).wait_send()
                return carry

            lax.fori_loop(0, z_count - 1, wait, 0)
            for d in range(1, handlers):
                fin_copy(slot, t, (me + d) % handlers, me).wait_send()

        handled(slot, sent)


def emit_kernel(*refs):
    sources, targets, sem = refs[:3], refs[3:6], refs[6]
    copies = [
        pltpu.make_async_copy(source, target, sem.at[i])
        for i, (source, target) in enumerate(zip(sources, targets))
    ]
    for copy in copies:
        copy.start()
    for copy in copies:
        copy.wait()


def per_device(sparse_vecs, dense_vec, top_cot, top_weight, owner_ids, local_rows, table, accum):
    batch_rows, table_count, width = sparse_vecs.shape
    rows_own = table.shape[1]
    z_count = lax.axis_size("dp") // 2
    mp_count = lax.axis_size("mp")
    handlers = 2 * mp_count
    slots = table_slots(table_count, handlers)
    count = len(slots)
    block = handlers * rows_own
    feature_count = table_count + 1
    dots = -(-feature_count * (SPAN // GROUP) // LANES)
    any_spec = pl.BlockSpec(memory_space=pl.ANY)
    hbm = pl.BlockSpec(memory_space=pltpu.HBM)
    vmem = pl.BlockSpec(memory_space=pltpu.VMEM)
    dma = pltpu.SemaphoreType.DMA
    bf16, f32, i32 = jnp.bfloat16, jnp.float32, jnp.int32
    out_shape = (
        jax.ShapeDtypeStruct(dense_vec.shape, bf16),
        jax.ShapeDtypeStruct(table.shape, f32),
        jax.ShapeDtypeStruct(accum.shape, f32),
    )
    scratch = [
        pltpu.VMEM((feature_count, batch_rows, width), bf16),
        pltpu.VMEM(top_cot.shape, bf16),
        pltpu.VMEM(top_weight.shape, bf16),
        pltpu.VMEM((table_count, 1, batch_rows), i32),
        pltpu.VMEM((table_count, batch_rows), i32),
        pltpu.VMEM(table.shape, f32),
        pltpu.VMEM(accum.shape, f32),
        pltpu.VMEM((handlers, count, 1, batch_rows), i32),
        pltpu.VMEM((feature_count * table_count // 2, dots * LANES), bf16),
        pltpu.VMEM((LANES, LANES // (SPAN // GROUP) * SPAN), bf16),
        pltpu.VMEM((batch_rows // GROUP, SPAN, width), bf16),
        pltpu.VMEM((batch_rows, dots * (LANES // (SPAN // GROUP)) * SPAN), f32),
        pltpu.VMEM((batch_rows, width), f32),
        pltpu.VMEM((table_count, batch_rows, width), bf16),
        pltpu.VMEM((count, handlers, batch_rows, width), bf16),
        pltpu.VMEM((handlers, count, 1, batch_rows), i32),
        pltpu.VMEM((count, z_count, block, width), bf16),
        pltpu.VMEM((count, block, width), f32),
        pltpu.VMEM((count, z_count, block, width), bf16),
        pltpu.VMEM((count, handlers, rows_own, width), bf16),
        pltpu.VMEM((table_count, rows_own, width), bf16),
        dma((8,)),
        dma((count,)),
        dma((handlers,)),
        dma((handlers,)),
        dma((count, handlers)),
        dma((count, handlers)),
        dma((count, z_count)),
        dma((count, z_count)),
        dma((count, handlers)),
        dma((count, handlers)),
    ]
    results = pl.pallas_call(
        functools.partial(step_kernel, slots, z_count, mp_count),
        out_shape=tuple(pltpu.VMEM(a.shape, a.dtype) for a in out_shape),
        in_specs=[hbm] * 8,
        out_specs=(vmem,) * 3,
        scratch_shapes=scratch,
        compiler_params=pltpu.CompilerParams(
            collective_id=0, has_side_effects=True, vmem_limit_bytes=VMEM_LIMIT
        ),
    )(
        sparse_vecs.transpose(1, 0, 2), dense_vec, top_cot, top_weight,
        owner_ids.transpose(1, 2, 0), local_rows.T, table, accum,
    )
    return pl.pallas_call(
        emit_kernel,
        out_shape=out_shape,
        in_specs=[vmem] * 3,
        out_specs=(any_spec,) * 3,
        scratch_shapes=[dma((3,))],
        compiler_params=pltpu.CompilerParams(vmem_limit_bytes=2 * 1024 * 1024),
    )(*results)


def solution(mesh):
    in_specs = (
        P(("dp", "mp"), None, None),
        P(("dp", "mp"), None),
        P(("dp", "mp"), None),
        P(),
        P(("dp", "mp"), None, None),
        P(("dp", "mp"), None),
        P(None, ("dp", "mp"), None),
        P(None, ("dp", "mp")),
    )
    out_specs = (P(("dp", "mp"), None), P(None, ("dp", "mp"), None), P(None, ("dp", "mp")))
    return jax.shard_map(
        per_device, mesh=mesh, in_specs=in_specs, out_specs=out_specs, check_vma=False
    )
```

```python
import functools

import jax
import jax.numpy as jnp
from jax import lax
from jax.experimental import pallas as pl
from jax.experimental.pallas import tpu as pltpu
from jax.sharding import PartitionSpec as P

LEARN_RATE = 0.1
EPSILON = 1e-08
MESH = pl.DeviceIdType.MESH
VMEM_LIMIT = 60 * 1024 * 1024
LANES = 128
GROUP = 8
SPAN = 256
UNROLL = 4
PARTS = (2, 14, 26)


def table_slots(table_count, handlers):
    slots = []
    rest = table_count % handlers
    starts = [0] * (rest > 0) + list(range(rest, table_count, handlers))
    for start in starts:
        count = rest if rest and start == 0 else handlers
        if count == handlers:
            slots.append((start, None))
        else:
            step = 2 if 2 * count <= handlers else 1
            owners = [handlers - step * (count - i) for i in range(count)]
            slots.append((start, tuple(owners)))
    return slots


def step_kernel(
    slots, z_count, mp_count,
    sparse, dense, cot, weight, owner, local, table, accum,
    dense_out, table_out, accum_out,
    feats, cot_v, weight_v, owner_v, local_v, table_v, accum_v,
    keys, select, repeat, blocks, spread, top, grads, got_rows, got_keys,
    partial, own_sum, z_in, fin_out, fin_in,
    load_sem, key_send, key_recv, row_send, row_recv,
    z_send, z_recv, fin_send, fin_recv,
):
    table_count, batch_rows, width = sparse.shape
    rows_own = table.shape[1]
    handlers = 2 * mp_count
    rows_grp = rows_own * mp_count
    block = handlers * rows_own
    feature_count = table_count + 1
    dp, mp = lax.axis_index("dp"), lax.axis_index("mp")
    z, x = dp // 2, dp % 2
    me = x * mp_count + mp

    def plane_device(h):
        return (z * 2 + h // mp_count, h % mp_count)

    def z_device(d):
        return (((z + d) % z_count) * 2 + x, mp)

    loads = [
        pltpu.make_async_copy(source, target, load_sem.at[i])
        for i, (source, target) in enumerate((
            (cot, cot_v), (weight, weight_v), (owner, owner_v), (local, local_v),
            (sparse, feats.at[pl.ds(0, table_count)]), (dense, feats.at[table_count]),
            (table, table_v), (accum, accum_v),
        ))
    ]
    for load in loads:
        load.start()

    peers = [plane_device((me + d) % handlers) for d in range(1, handlers)]
    peers_z = [z_device(d) for d in range(1, z_count)]
    barrier = pltpu.get_barrier_semaphore()
    for device in peers + peers_z:
        pl.semaphore_signal(barrier, inc=1, device_id=device, device_id_type=MESH)

    with jax.named_scope("const"):
        pair_count = feature_count * (feature_count - 1) // 2
        feature_pad = SPAN // GROUP
        per_dot = LANES // feature_pad
        dots = -(-feature_count // per_dot)
        columns = lax.broadcasted_iota(jnp.int32, (1, dots * LANES), 1)
        left, right = columns // feature_pad, columns % feature_pad
        inside = (left < feature_count) & (right < feature_count) & (left != right)
        left = jnp.where(left == table_count, 0, left + 1)
        right = jnp.where(right == table_count, 0, right + 1)
        high, low = jnp.maximum(left, right), jnp.minimum(left, right)
        place = jnp.where(inside, high * (high - 1) // 2 + low, -1)
        pairs = lax.broadcasted_iota(jnp.int32, (pair_count, dots * LANES), 0)
        select[...] = jnp.where(pairs == place, 1.0, 0.0).astype(jnp.bfloat16)
        rep_row = lax.broadcasted_iota(jnp.int32, (LANES, per_dot * SPAN), 0)
        rep_col = lax.broadcasted_iota(jnp.int32, (LANES, per_dot * SPAN), 1)
        repeat[...] = jnp.where(rep_row == rep_col // GROUP, 1.0, 0.0).astype(jnp.bfloat16)
    with jax.named_scope("loadwait"):
        loads[0].wait()
        loads[1].wait()
    input_cot = lax.dot_general(
        cot_v[...], weight_v[...], (((1,), (1,)), ((), ())), preferred_element_type=jnp.float32
    )
    top[...] = input_cot[:, :width]
    symmetric = jnp.dot(
        input_cot[:, width:].astype(jnp.bfloat16), select[...], preferred_element_type=jnp.float32
    ).astype(jnp.bfloat16)

    loads[4].wait()
    loads[5].wait()

    def build_blocks(i, carry):
        span = pl.ds(pl.multiple_of(i * 2 * GROUP, 2 * GROUP), 2 * GROUP)
        both = feats[:, span, :].astype(jnp.float32)
        pad = jnp.zeros(((feature_pad - feature_count) * GROUP, width), jnp.float32)
        for half in range(2):
            part = both[:, half * GROUP : (half + 1) * GROUP, :]
            part = part.reshape(feature_count * GROUP, width)
            blocks[2 * i + half] = jnp.concatenate([part, pad], 0).astype(jnp.bfloat16)
        return carry

    with jax.named_scope("blocks"):
        lax.fori_loop(0, batch_rows // (2 * GROUP), build_blocks, 0)

    mask = (
        lax.broadcasted_iota(jnp.int32, (GROUP, SPAN), 1) % GROUP
        == lax.broadcasted_iota(jnp.int32, (GROUP, SPAN), 0)
    )

    def gradients(first, last):
        for q in range(first // per_dot, -(-last // per_dot)):
            spread[:, q * per_dot * SPAN : (q + 1) * per_dot * SPAN] = jnp.dot(
                symmetric[:, q * LANES : (q + 1) * LANES], repeat[...],
                preferred_element_type=jnp.float32,
            )

        def one(step, carry):
            for i in [step * UNROLL + u for u in range(UNROLL)]:
                outs = []
                for half in range(2):
                    rows = pl.ds(pl.multiple_of((2 * i + half) * GROUP, GROUP), GROUP)
                    parts = [
                        jnp.where(mask, spread[rows, t * SPAN : (t + 1) * SPAN], 0.0)
                        for t in range(first, last)
                    ]
                    lhs = jnp.concatenate(parts, 0).astype(jnp.bfloat16)
                    outs.append(
                        jnp.dot(lhs, blocks[2 * i + half], preferred_element_type=jnp.float32)
                    )
                span = pl.ds(pl.multiple_of(i * 2 * GROUP, 2 * GROUP), 2 * GROUP)
                for t in range(first, last):
                    at = (t - first) * GROUP
                    both = jnp.concatenate([out[at : at + GROUP] for out in outs], 0)
                    if t == table_count:
                        dense_out[span, :] = (both + top[span, :]).astype(jnp.bfloat16)
                    else:
                        grads[t, span, :] = both.astype(jnp.bfloat16)
            return carry

        lax.fori_loop(0, batch_rows // (2 * GROUP * UNROLL), one, 0)

    def table_of(slot, h):
        return slots[slot][0] + h // 2 + (h % 2) * (handlers // 2)

    def all_in(buffer, sem):
        pltpu.make_async_copy(buffer, buffer, sem).wait()

    def row_copy(slot, t, target, source):
        return pltpu.make_async_remote_copy(
            src_ref=grads.at[t],
            dst_ref=got_rows.at[slot, source],
            send_sem=row_send.at[slot],
            recv_sem=row_recv.at[slot],
            device_id=plane_device(target),
            device_id_type=MESH,
        )

    def key_copy(target, source):
        return pltpu.make_async_remote_copy(
            src_ref=keys.at[target],
            dst_ref=got_keys.at[source],
            send_sem=key_send,
            recv_sem=key_recv,
            device_id=plane_device(target),
            device_id_type=MESH,
        )

    def self_copy(slot, t):
        return pltpu.make_async_copy(grads.at[t], got_rows.at[slot, me], row_recv.at[slot])

    def targets_of(slot, parity):
        start, owners = slots[slot]
        if owners is None:
            for j in range(1, handlers // 2):
                h = 2 * ((me // 2 + j) % (handlers // 2)) + parity
                yield h, table_of(slot, h), None
            h = 2 * (me // 2) + parity
            yield h, table_of(slot, h), me != h
        else:
            for i, h in enumerate(owners):
                if h % 2 == parity:
                    yield h, start + i, me != h

    def guarded(condition, body):
        if condition is None:
            body()
        else:
            pl.when(condition)(body)

    def handled(slot, body, parity=None):
        start, owners = slots[slot]
        if owners is None:
            if parity is None:
                body(table_of(slot, me))
            else:
                guarded(me % 2 == parity, lambda: body(table_of(slot, me)))
        else:
            for i, h in enumerate(owners):
                if parity is None or h % 2 == parity:
                    guarded(me == h, lambda i=i: body(start + i))

    def send_rows(slot, parity):
        for h, t, condition in targets_of(slot, parity):
            guarded(condition, lambda: row_copy(slot, t, h, me).start())
        handled(slot, lambda t: self_copy(slot, t).start(), parity)

    def build_keys():
        for slot, (start, owners) in enumerate(slots):
            for h in range(handlers):
                if owners is None:
                    t = table_of(slot, h)
                else:
                    t = start + (owners.index(h) if h in owners else 0)
                keys[h, slot] = owner_v[t] * rows_grp + local_v[t : t + 1]
        for slot in range(len(slots)):
            got_keys[me, slot] = keys[me, slot]

    def send_keys():
        for d in range(1, handlers):
            key_copy((me + d) % handlers, me).start()

    def wait_sent(slot):
        start, owners = slots[slot]
        if owners is None:
            all_in(grads.at[pl.ds(0, handlers - 1)], row_send.at[slot])
        else:
            mine = [me == h for h in owners]
            mine = functools.reduce(jnp.logical_or, mine)
            for less in range(2):
                sent = len(owners) - less
                if sent:
                    guarded(
                        mine if less else jnp.logical_not(mine),
                        lambda: all_in(grads.at[pl.ds(0, sent)], row_send.at[slot]),
                    )

    def z_order(step):
        low = z_count - 1 - step
        low = low - jnp.where(low <= z, 1, 0)
        high = step + jnp.where(step >= z, 1, 0)
        return jnp.where(2 * z < z_count, low, high)

    def z_copy(slot, target, source):
        return pltpu.make_async_remote_copy(
            src_ref=partial.at[slot, target],
            dst_ref=z_in.at[slot, source],
            send_sem=z_send.at[slot],
            recv_sem=z_recv.at[slot],
            device_id=(target * 2 + x, mp),
            device_id_type=MESH,
        )

    def job(slot):
        def body(t):
            with jax.named_scope(f"jobwait{slot}"):
                all_in(got_rows.at[slot], row_recv.at[slot])
            targets = lax.broadcasted_iota(jnp.int32, (block, batch_rows), 0)

            def sums(target):
                base = target * block
                total = jnp.zeros((block, width), jnp.float32)
                for h in range(handlers):
                    onehot = jnp.where(targets == got_keys[h, slot] - base, 1.0, 0.0)
                    total = total + jnp.dot(
                        onehot.astype(jnp.bfloat16), got_rows[slot, h],
                        preferred_element_type=jnp.float32,
                    )
                return total

            def away(step, carry):
                target = z_order(step)
                partial[slot, target] = sums(target).astype(jnp.bfloat16)
                z_copy(slot, target, z).start()
                return carry

            lax.fori_loop(0, z_count - 1, away, 0)
            own_sum[slot] = sums(z)

        handled(slot, body)

    def fin_copy(slot, t, target, source):
        return pltpu.make_async_remote_copy(
            src_ref=fin_out.at[slot, target],
            dst_ref=fin_in.at[t],
            send_sem=fin_send.at[slot],
            recv_sem=fin_recv.at[slot],
            device_id=plane_device(target),
            device_id_type=MESH,
        )

    def finish(slot):
        def body(t):
            with jax.named_scope(f"finwait{slot}"):
                if z_count > 1:
                    all_in(z_in.at[slot, pl.ds(0, z_count - 1)], z_recv.at[slot])
            total = own_sum[slot]
            for d in range(1, z_count):
                total = total + z_in[slot, (z + d) % z_count].astype(jnp.float32)
            total = total.astype(jnp.bfloat16)
            for h in range(handlers):
                fin_out[slot, h] = total[h * rows_own : (h + 1) * rows_own]
            for d in range(1, handlers):
                fin_copy(slot, t, (me + d) % handlers, me).start()
            fin_in[t] = fin_out[slot, me]

        handled(slot, body)

    lane = lax.broadcasted_iota(jnp.int32, (rows_own, LANES), 1)
    state = {}

    def update(slot):
        start, owners = slots[slot]
        count = handlers if owners is None else len(owners)
        if owners is None:
            all_in(fin_in.at[pl.ds(0, handlers - 1)], fin_recv.at[slot])
        else:
            mine = functools.reduce(jnp.logical_or, [me == h for h in owners])
            for less in range(2):
                came = count - less
                if came:
                    guarded(
                        mine if less else jnp.logical_not(mine),
                        lambda: all_in(fin_in.at[pl.ds(0, came)], fin_recv.at[slot]),
                    )
        span = slice(start, start + count)
        grad = fin_in[span].astype(jnp.float32)
        mean = jnp.sum(grad * grad, axis=2, keepdims=True) * (1.0 / width)
        old = jnp.stack([state["old"][:, t : t + 1] for t in range(start, start + count)])
        new = old + mean
        for i in range(count):
            state["new"] = jnp.where(lane == start + i, new[i], state["new"])
        table_out[span] = table_v[span] - grad * (LEARN_RATE / (jnp.sqrt(new) + EPSILON))

    def rows_of(slot):
        start, owners = slots[slot]
        return start, start + (handlers if owners is None else len(owners))

    count = len(slots)
    sends = []
    for slot in range(count):
        first, last = rows_of(slot)
        if slots[slot][1] is None:
            sends += [(slot, 0, first + handlers // 2), (slot, 1, last)]
        else:
            sends += [(slot, 0, last), (slot, 1, last)]
    done = 0
    for part, last in enumerate(PARTS):
        last = min(last, table_count)
        if part == len(PARTS) - 1:
            last = table_count
        with jax.named_scope(f"grad{part}"):
            gradients(done, last + (1 if last == table_count else 0))
        if part == 0:
            loads[2].wait()
            loads[3].wait()
            build_keys()
            with jax.named_scope("barrier"):
                pl.semaphore_wait(barrier, handlers - 1 + z_count - 1)
            send_keys()
        for slot, parity, ready in sends:
            if done < ready <= last or (parity and ready == last == table_count):
                send_rows(slot, parity)
        done = last

    loads[6].wait()
    loads[7].wait()
    old = jnp.concatenate(
        [accum_v[...], jnp.zeros((LANES - table_count, rows_own), jnp.float32)], 0
    )
    state["old"] = old.T
    state["new"] = jnp.zeros((rows_own, LANES), jnp.float32)

    all_in(got_keys.at[pl.ds(0, handlers - 1)], key_recv)

    plan = []
    for step in range(count + 1):
        plan += [(job, step)] * (step < count) + [(finish, step - 1)] * (step > 0)
    last = plan.pop()
    plan += [(update, slot) for slot in range(count - 2)] + [last]
    plan += [(update, slot) for slot in range(max(0, count - 2), count)]
    for stage, slot in plan:
        with jax.named_scope(f"{stage.__name__}{slot}"):
            stage(slot)
    with jax.named_scope("accum"):
        accum_out[...] = state["new"].T[:table_count]

    all_in(keys.at[pl.ds(0, handlers - 1)], key_send)
    for slot in range(count):
      with jax.named_scope("sent"):
        wait_sent(slot)

        def sent(t):
            if z_count > 1:
                all_in(partial.at[slot, pl.ds(0, z_count - 1)], z_send.at[slot])
            all_in(fin_out.at[slot, pl.ds(0, handlers - 1)], fin_send.at[slot])

        handled(slot, sent)


def emit_kernel(*refs):
    sources, targets, sem = refs[:3], refs[3:6], refs[6]
    copies = [
        pltpu.make_async_copy(source, target, sem.at[i])
        for i, (source, target) in enumerate(zip(sources, targets))
    ]
    for copy in copies:
        copy.start()
    for copy in copies:
        copy.wait()


def per_device(sparse_vecs, dense_vec, top_cot, top_weight, owner_ids, local_rows, table, accum):
    batch_rows, table_count, width = sparse_vecs.shape
    rows_own = table.shape[1]
    z_count = lax.axis_size("dp") // 2
    mp_count = lax.axis_size("mp")
    handlers = 2 * mp_count
    slots = table_slots(table_count, handlers)
    count = len(slots)
    block = handlers * rows_own
    feature_count = table_count + 1
    dots = -(-feature_count * (SPAN // GROUP) // LANES)
    any_spec = pl.BlockSpec(memory_space=pl.ANY)
    hbm = pl.BlockSpec(memory_space=pltpu.HBM)
    vmem = pl.BlockSpec(memory_space=pltpu.VMEM)
    dma = pltpu.SemaphoreType.DMA
    bf16, f32, i32 = jnp.bfloat16, jnp.float32, jnp.int32
    out_shape = (
        jax.ShapeDtypeStruct(dense_vec.shape, bf16),
        jax.ShapeDtypeStruct(table.shape, f32),
        jax.ShapeDtypeStruct(accum.shape, f32),
    )
    scratch = [
        pltpu.VMEM((feature_count, batch_rows, width), bf16),
        pltpu.VMEM(top_cot.shape, bf16),
        pltpu.VMEM(top_weight.shape, bf16),
        pltpu.VMEM((table_count, 1, batch_rows), i32),
        pltpu.VMEM((table_count, batch_rows), i32),
        pltpu.VMEM(table.shape, f32),
        pltpu.VMEM(accum.shape, f32),
        pltpu.VMEM((handlers, count, 1, batch_rows), i32),
        pltpu.VMEM((feature_count * table_count // 2, dots * LANES), bf16),
        pltpu.VMEM((LANES, LANES // (SPAN // GROUP) * SPAN), bf16),
        pltpu.VMEM((batch_rows // GROUP, SPAN, width), bf16),
        pltpu.VMEM((batch_rows, dots * (LANES // (SPAN // GROUP)) * SPAN), f32),
        pltpu.VMEM((batch_rows, width), f32),
        pltpu.VMEM((table_count, batch_rows, width), bf16),
        pltpu.VMEM((count, handlers, batch_rows, width), bf16),
        pltpu.VMEM((handlers, count, 1, batch_rows), i32),
        pltpu.VMEM((count, z_count, block, width), bf16),
        pltpu.VMEM((count, block, width), f32),
        pltpu.VMEM((count, z_count, block, width), bf16),
        pltpu.VMEM((count, handlers, rows_own, width), bf16),
        pltpu.VMEM((table_count, rows_own, width), bf16),
        dma((8,)),
        dma,
        dma,
    ] + [dma((count,)) for _ in range(6)]
    results = pl.pallas_call(
        functools.partial(step_kernel, slots, z_count, mp_count),
        out_shape=tuple(pltpu.VMEM(a.shape, a.dtype) for a in out_shape),
        in_specs=[hbm] * 8,
        out_specs=(vmem,) * 3,
        scratch_shapes=scratch,
        compiler_params=pltpu.CompilerParams(
            collective_id=0, has_side_effects=True, vmem_limit_bytes=VMEM_LIMIT
        ),
    )(
        sparse_vecs.transpose(1, 0, 2), dense_vec, top_cot, top_weight,
        owner_ids.transpose(1, 2, 0), local_rows.T, table, accum,
    )
    return pl.pallas_call(
        emit_kernel,
        out_shape=out_shape,
        in_specs=[vmem] * 3,
        out_specs=(any_spec,) * 3,
        scratch_shapes=[dma((3,))],
        compiler_params=pltpu.CompilerParams(vmem_limit_bytes=2 * 1024 * 1024),
    )(*results)


def solution(mesh):
    in_specs = (
        P(("dp", "mp"), None, None),
        P(("dp", "mp"), None),
        P(("dp", "mp"), None),
        P(),
        P(("dp", "mp"), None, None),
        P(("dp", "mp"), None),
        P(None, ("dp", "mp"), None),
        P(None, ("dp", "mp")),
    )
    out_specs = (P(("dp", "mp"), None), P(None, ("dp", "mp"), None), P(None, ("dp", "mp")))
    return jax.shard_map(
        per_device, mesh=mesh, in_specs=in_specs, out_specs=out_specs, check_vma=False
    )
```

```python
import functools

import jax
import jax.numpy as jnp
from jax import lax
from jax.experimental import pallas as pl
from jax.experimental.pallas import tpu as pltpu
from jax.sharding import PartitionSpec as P

LEARN_RATE = 0.1
EPSILON = 1e-08
MESH = pl.DeviceIdType.MESH
VMEM_LIMIT = 60 * 1024 * 1024
LANES = 128
GROUP = 8
SPAN = 256
UNROLL = 4
PARTS = (4, 10, 26)


def table_slots(table_count, handlers):
    slots = []
    rest = table_count % handlers
    counts = [handlers] * (table_count // handlers)
    if rest:
        counts.insert(min(1, len(counts)), rest)
    start = 0
    for count in counts:
        if count == handlers:
            slots.append((start, None))
        else:
            step = 2 if 2 * count <= handlers else 1
            owners = [handlers - step * (count - i) for i in range(count)]
            slots.append((start, tuple(owners)))
        start += count
    return slots


def step_kernel(
    slots, direct, z_count, mp_count,
    sparse, dense, cot, weight, owner, local, table, accum,
    dense_out, table_out, accum_out,
    cot_v, weight_v, owner_v, local_v, table_v, accum_v,
    keys, pair_cot, select, repeat, blocks, spread, top, grads, got_rows, got_keys,
    partial, own_sum, z_in, fin_out, fin_in, pieces,
    load_sem, tile_sem, key_send, key_recv, row_send, row_recv,
    z_send, z_recv, fin_send, fin_recv, direct_send, direct_recv,
):
    table_count, groups, _, width = sparse.shape
    batch_rows = groups * GROUP
    rows_own = table.shape[1]
    handlers = 2 * mp_count
    rows_grp = rows_own * mp_count
    block = handlers * rows_own
    feature_count = table_count + 1
    dp, mp = lax.axis_index("dp"), lax.axis_index("mp")
    z, x = dp // 2, dp % 2
    me = x * mp_count + mp

    def plane_device(h):
        return (z * 2 + h // mp_count, h % mp_count)

    def z_device(d):
        return (((z + d) % z_count) * 2 + x, mp)

    def all_in(buffer, sem):
        pltpu.make_async_copy(buffer, buffer, sem).wait()

    loads = [
        pltpu.make_async_copy(source, target, load_sem.at[i])
        for i, (source, target) in enumerate((
            (cot, cot_v), (weight, weight_v), (owner, owner_v), (local, local_v),
            (dense, blocks.at[:, table_count]), (table, table_v), (accum, accum_v),
        ))
    ]
    tiles = [
        pltpu.make_async_copy(
            sparse.at[:, g], blocks.at[g, pl.ds(0, table_count)],
            tile_sem.at[g // (2 * UNROLL)],
        )
        for g in range(groups)
    ]
    for load in loads[:4]:
        load.start()
    blocks[:, pl.ds(feature_count, SPAN // GROUP - feature_count)] = jnp.zeros(
        (groups, SPAN // GROUP - feature_count, GROUP, width), jnp.bfloat16
    )

    barrier = pltpu.get_barrier_semaphore()
    device_count = 2 * z_count * mp_count

    def greet(step, carry):
        other = (dp * mp_count + mp + 1 + step) % device_count
        pl.semaphore_signal(
            barrier, inc=1, device_id=(other // mp_count, other % mp_count),
            device_id_type=MESH,
        )
        return carry

    lax.fori_loop(0, device_count - 1, greet, 0)

    with jax.named_scope("const"):
        pair_count = feature_count * (feature_count - 1) // 2
        feature_pad = SPAN // GROUP
        per_dot = LANES // feature_pad
        dots = -(-feature_count // per_dot)
        columns = lax.broadcasted_iota(jnp.int32, (1, dots * LANES), 1)
        left, right = columns // feature_pad, columns % feature_pad
        inside = (left < feature_count) & (right < feature_count) & (left != right)
        left = jnp.where(left == table_count, 0, left + 1)
        right = jnp.where(right == table_count, 0, right + 1)
        high, low = jnp.maximum(left, right), jnp.minimum(left, right)
        place = jnp.where(inside, high * (high - 1) // 2 + low, -1)
        pairs = lax.broadcasted_iota(jnp.int32, (pair_count, dots * LANES), 0)
        select[...] = jnp.where(pairs == place, 1.0, 0.0).astype(jnp.bfloat16)
        rep_row = lax.broadcasted_iota(jnp.int32, (LANES, per_dot * SPAN), 0)
        rep_col = lax.broadcasted_iota(jnp.int32, (LANES, per_dot * SPAN), 1)
        repeat[...] = jnp.where(rep_row == rep_col // GROUP, 1.0, 0.0).astype(jnp.bfloat16)
    with jax.named_scope("loadwait"):
        loads[0].wait()
        for load in loads[4:5] + tiles + loads[5:]:
            load.start()
        loads[1].wait()
    input_cot = lax.dot_general(
        cot_v[...], weight_v[...], (((1,), (1,)), ((), ())), preferred_element_type=jnp.float32
    )
    top[...] = input_cot[:, :width]
    pair_cot[...] = input_cot[:, width:].astype(jnp.bfloat16)

    with jax.named_scope("blocks"):
        loads[4].wait()

    features = blocks.reshape(groups, SPAN, width)
    mask = (
        lax.broadcasted_iota(jnp.int32, (GROUP, SPAN), 1) % GROUP
        == lax.broadcasted_iota(jnp.int32, (GROUP, SPAN), 0)
    )

    def gradients(first, last):
        for q in range(-(-first // per_dot), -(-last // per_dot)):
            symmetric = jnp.dot(
                pair_cot[...], select[:, q * LANES : (q + 1) * LANES],
                preferred_element_type=jnp.float32,
            ).astype(jnp.bfloat16)
            spread[:, q * per_dot * SPAN : (q + 1) * per_dot * SPAN] = jnp.dot(
                symmetric, repeat[...], preferred_element_type=jnp.float32
            )

        def one(step, carry):
            if first == 0:
                span = pl.ds(step * 2 * UNROLL, 2 * UNROLL)
                all_in(blocks.at[span, pl.ds(0, table_count)], tile_sem.at[step])
            for i in [step * UNROLL + u for u in range(UNROLL)]:
                outs = []
                for half in range(2):
                    rows = pl.ds(pl.multiple_of((2 * i + half) * GROUP, GROUP), GROUP)
                    parts = [
                        jnp.where(mask, spread[rows, t * SPAN : (t + 1) * SPAN], 0.0)
                        for t in range(first, last)
                    ]
                    lhs = jnp.concatenate(parts, 0).astype(jnp.bfloat16)
                    outs.append(
                        jnp.dot(lhs, features[2 * i + half], preferred_element_type=jnp.float32)
                    )
                span = pl.ds(pl.multiple_of(i * 2 * GROUP, 2 * GROUP), 2 * GROUP)
                for t in range(first, last):
                    at = (t - first) * GROUP
                    both = jnp.concatenate([out[at : at + GROUP] for out in outs], 0)
                    if t == table_count:
                        dense_out[span, :] = (both + top[span, :]).astype(jnp.bfloat16)
                    else:
                        grads[t, span, :] = both.astype(jnp.bfloat16)
            return carry

        lax.fori_loop(0, batch_rows // (2 * GROUP * UNROLL), one, 0)

    def table_of(slot, h):
        return slots[slot][0] + h // 2 + (h % 2) * (handlers // 2)

    def row_copy(slot, t, target, source):
        return pltpu.make_async_remote_copy(
            src_ref=grads.at[t],
            dst_ref=got_rows.at[slot, source],
            send_sem=row_send.at[slot],
            recv_sem=row_recv.at[slot],
            device_id=plane_device(target),
            device_id_type=MESH,
        )

    def key_copy(target, source):
        return pltpu.make_async_remote_copy(
            src_ref=keys.at[target],
            dst_ref=got_keys.at[source],
            send_sem=key_send,
            recv_sem=key_recv,
            device_id=plane_device(target),
            device_id_type=MESH,
        )

    def self_copy(slot, t):
        return pltpu.make_async_copy(grads.at[t], got_rows.at[slot, me], row_recv.at[slot])

    def targets_of(slot, parity):
        start, owners = slots[slot]
        if owners is None:
            for j in range(1, handlers // 2):
                h = 2 * ((me // 2 + j) % (handlers // 2)) + parity
                yield h, table_of(slot, h), None
            h = 2 * (me // 2) + parity
            yield h, table_of(slot, h), me != h
        else:
            for i, h in enumerate(owners):
                if h % 2 == parity:
                    yield h, start + i, me != h

    def guarded(condition, body):
        if condition is None:
            body()
        else:
            pl.when(condition)(body)

    def handled(slot, body, parity=None):
        start, owners = slots[slot]
        if owners is None:
            if parity is None:
                body(table_of(slot, me))
            else:
                guarded(me % 2 == parity, lambda: body(table_of(slot, me)))
        else:
            for i, h in enumerate(owners):
                if parity is None or h % 2 == parity:
                    guarded(me == h, lambda i=i: body(start + i))

    def send_rows(slot, parity):
        for h, t, condition in targets_of(slot, parity):
            guarded(condition, lambda: row_copy(slot, t, h, me).start())
        handled(slot, lambda t: self_copy(slot, t).start(), parity)

    def build_keys():
        for slot, (start, owners) in enumerate(slots):
            for h in range(handlers):
                if owners is None:
                    t = table_of(slot, h)
                else:
                    t = start + (owners.index(h) if h in owners else 0)
                keys[h, slot] = owner_v[t] * rows_grp + local_v[t : t + 1]
        for slot in range(len(slots)):
            got_keys[me, slot] = keys[me, slot]

    def send_keys():
        for d in range(1, handlers):
            key_copy((me + d) % handlers, me).start()

    def wait_sent(slot):
        start, owners = slots[slot]
        if owners is None:
            all_in(grads.at[pl.ds(0, handlers - 1)], row_send.at[slot])
        else:
            mine = [me == h for h in owners]
            mine = functools.reduce(jnp.logical_or, mine)
            for less in range(2):
                sent = len(owners) - less
                if sent:
                    guarded(
                        mine if less else jnp.logical_not(mine),
                        lambda: all_in(grads.at[pl.ds(0, sent)], row_send.at[slot]),
                    )

    def z_order(step):
        low = z_count - 1 - step
        low = low - jnp.where(low <= z, 1, 0)
        high = step + jnp.where(step >= z, 1, 0)
        return jnp.where(2 * z < z_count, low, high)

    def z_copy(slot, target, source):
        return pltpu.make_async_remote_copy(
            src_ref=partial.at[slot, target],
            dst_ref=z_in.at[slot, source],
            send_sem=z_send.at[slot],
            recv_sem=z_recv.at[slot],
            device_id=(target * 2 + x, mp),
            device_id_type=MESH,
        )

    def direct_copy(slot, target, h):
        return pltpu.make_async_remote_copy(
            src_ref=partial.at[slot, target, pl.ds(pl.multiple_of(h * rows_own, 16), rows_own)],
            dst_ref=pieces.at[me * z_count + z],
            send_sem=direct_send,
            recv_sem=direct_recv,
            device_id=(target * 2 + h // mp_count, h % mp_count),
            device_id_type=MESH,
        )

    def job(slot):
        def body(t):
            with jax.named_scope(f"jobwait{slot}"):
                all_in(got_rows.at[slot], row_recv.at[slot])
            targets = lax.broadcasted_iota(jnp.int32, (block, batch_rows), 0)

            def sums(target):
                base = target * block
                total = jnp.zeros((block, width), jnp.float32)
                for h in range(handlers):
                    onehot = jnp.where(targets == got_keys[h, slot] - base, 1.0, 0.0)
                    total = total + jnp.dot(
                        onehot.astype(jnp.bfloat16), got_rows[slot, h],
                        preferred_element_type=jnp.float32,
                    )
                return total

            def away(step, carry):
                target = z_order(step)
                partial[slot, target] = sums(target).astype(jnp.bfloat16)
                if slot == direct:
                    for h in range(handlers):
                        direct_copy(slot, target, h).start()
                else:
                    z_copy(slot, target, z).start()
                return carry

            lax.fori_loop(0, z_count - 1, away, 0)
            if slot == direct:
                partial[slot, z] = sums(z).astype(jnp.bfloat16)
                for d in range(1, handlers):
                    direct_copy(slot, z, (me + d) % handlers).start()
                span = pl.ds(pl.multiple_of(me * rows_own, 16), rows_own)
                pieces[me * z_count + z] = partial[slot, z, span]
            else:
                own_sum[slot] = sums(z)

        handled(slot, body)

    def fin_copy(slot, t, target, source):
        return pltpu.make_async_remote_copy(
            src_ref=fin_out.at[slot, target],
            dst_ref=fin_in.at[t],
            send_sem=fin_send.at[slot],
            recv_sem=fin_recv.at[slot],
            device_id=plane_device(target),
            device_id_type=MESH,
        )

    def finish(slot):
        def body(t):
            with jax.named_scope(f"finwait{slot}"):
                if z_count > 1:
                    all_in(z_in.at[slot, pl.ds(0, z_count - 1)], z_recv.at[slot])
            total = own_sum[slot]
            for d in range(1, z_count):
                total = total + z_in[slot, (z + d) % z_count].astype(jnp.float32)
            total = total.astype(jnp.bfloat16)
            for h in range(handlers):
                fin_out[slot, h] = total[h * rows_own : (h + 1) * rows_own]
            for d in range(1, handlers):
                fin_copy(slot, t, (me + d) % handlers, me).start()
            fin_in[t] = fin_out[slot, me]

        handled(slot, body)

    lane = lax.broadcasted_iota(jnp.int32, (rows_own, LANES), 1)
    state = {}

    def update(slot):
        start, owners = slots[slot]
        count = handlers if owners is None else len(owners)
        span = slice(start, start + count)
        if slot == direct:
            all_in(pieces.at[pl.ds(0, handlers * z_count - 1)], direct_recv)
            parts = [None] * handlers
            for h in range(handlers):
                total = pieces[h * z_count].astype(jnp.float32)
                for source in range(1, z_count):
                    total = total + pieces[h * z_count + source].astype(jnp.float32)
                parts[table_of(0, h) - slots[0][0]] = total
            grad = jnp.stack(parts)
        elif owners is None:
            all_in(fin_in.at[pl.ds(0, handlers - 1)], fin_recv.at[slot])
        else:
            mine = functools.reduce(jnp.logical_or, [me == h for h in owners])
            for less in range(2):
                came = count - less
                if came:
                    guarded(
                        mine if less else jnp.logical_not(mine),
                        lambda: all_in(fin_in.at[pl.ds(0, came)], fin_recv.at[slot]),
                    )
        if slot != direct:
            grad = fin_in[span].astype(jnp.float32)
        mean = jnp.sum(grad * grad, axis=2, keepdims=True) * (1.0 / width)
        old = jnp.stack([state["old"][:, t : t + 1] for t in range(start, start + count)])
        new = old + mean
        for i in range(count):
            state["new"] = jnp.where(lane == start + i, new[i], state["new"])
        table_out[span] = table_v[span] - grad * (LEARN_RATE / (jnp.sqrt(new) + EPSILON))

    def rows_of(slot):
        start, owners = slots[slot]
        return start, start + (handlers if owners is None else len(owners))

    count = len(slots)
    sends = []
    for slot in range(count):
        first, last = rows_of(slot)
        if slots[slot][1] is None:
            sends += [(slot, 0, first + handlers // 2), (slot, 1, last)]
        else:
            sends += [(slot, 0, last), (slot, 1, last)]
    done = 0
    for part, last in enumerate(PARTS):
        last = min(last, table_count)
        if part == len(PARTS) - 1:
            last = table_count
        with jax.named_scope(f"grad{part}"):
            gradients(done, last + (1 if last == table_count else 0))
        if part == 0:
            loads[2].wait()
            loads[3].wait()
            build_keys()
            with jax.named_scope("barrier"):
                pl.semaphore_wait(barrier, device_count - 1)
            send_keys()
        for slot, parity, ready in sends:
            if done < ready <= last or (parity and ready == last == table_count):
                send_rows(slot, parity)
        done = last

    loads[5].wait()
    loads[6].wait()
    old = jnp.concatenate(
        [accum_v[...], jnp.zeros((LANES - table_count, rows_own), jnp.float32)], 0
    )
    state["old"] = old.T
    state["new"] = jnp.zeros((rows_own, LANES), jnp.float32)

    all_in(got_keys.at[pl.ds(0, handlers - 1)], key_recv)

    plan = []
    for step in range(count + 1):
        plan += [(job, step)] * (step < count) + [(finish, step - 1)] * (step > 0)
    plan += [(update, slot) for slot in range(count)]
    plan = [(stage, slot) for stage, slot in plan if stage is not finish or slot != direct]
    for stage, slot in plan:
        with jax.named_scope(f"{stage.__name__}{slot}"):
            stage(slot)
    with jax.named_scope("accum"):
        accum_out[...] = state["new"].T[:table_count]

    all_in(keys.at[pl.ds(0, handlers - 1)], key_send)
    for slot in range(count):
      with jax.named_scope("sent"):
        wait_sent(slot)

        def sent(t):
            if slot == direct:
                all_in(pieces.at[pl.ds(0, handlers * z_count - 1)], direct_send)
                return
            if z_count > 1:
                all_in(partial.at[slot, pl.ds(0, z_count - 1)], z_send.at[slot])
            all_in(fin_out.at[slot, pl.ds(0, handlers - 1)], fin_send.at[slot])

        handled(slot, sent)


def emit_kernel(*refs):
    sources, targets, sem = refs[:3], refs[3:6], refs[6]
    copies = [
        pltpu.make_async_copy(source, target, sem.at[i])
        for i, (source, target) in enumerate(zip(sources, targets))
    ]
    for copy in copies:
        copy.start()
    for copy in copies:
        copy.wait()


def per_device(sparse_vecs, dense_vec, top_cot, top_weight, owner_ids, local_rows, table, accum):
    batch_rows, table_count, width = sparse_vecs.shape
    rows_own = table.shape[1]
    groups = batch_rows // GROUP
    z_count = lax.axis_size("dp") // 2
    mp_count = lax.axis_size("mp")
    handlers = 2 * mp_count
    slots = table_slots(table_count, handlers)
    count = len(slots)
    direct = count - 1 if slots[count - 1][1] is None else None
    block = handlers * rows_own
    feature_count = table_count + 1
    dots = -(-feature_count * (SPAN // GROUP) // LANES)
    any_spec = pl.BlockSpec(memory_space=pl.ANY)
    hbm = pl.BlockSpec(memory_space=pltpu.HBM)
    vmem = pl.BlockSpec(memory_space=pltpu.VMEM)
    dma = pltpu.SemaphoreType.DMA
    bf16, f32, i32 = jnp.bfloat16, jnp.float32, jnp.int32
    out_shape = (
        jax.ShapeDtypeStruct(dense_vec.shape, bf16),
        jax.ShapeDtypeStruct(table.shape, f32),
        jax.ShapeDtypeStruct(accum.shape, f32),
    )
    scratch = [
        pltpu.VMEM(top_cot.shape, bf16),
        pltpu.VMEM(top_weight.shape, bf16),
        pltpu.VMEM((table_count, 1, batch_rows), i32),
        pltpu.VMEM((table_count, batch_rows), i32),
        pltpu.VMEM(table.shape, f32),
        pltpu.VMEM(accum.shape, f32),
        pltpu.VMEM((handlers, count, 1, batch_rows), i32),
        pltpu.VMEM((batch_rows, feature_count * table_count // 2), bf16),
        pltpu.VMEM((feature_count * table_count // 2, dots * LANES), bf16),
        pltpu.VMEM((LANES, LANES // (SPAN // GROUP) * SPAN), bf16),
        pltpu.VMEM((groups, SPAN // GROUP, GROUP, width), bf16),
        pltpu.VMEM((batch_rows, dots * (LANES // (SPAN // GROUP)) * SPAN), f32),
        pltpu.VMEM((batch_rows, width), f32),
        pltpu.VMEM((table_count, batch_rows, width), bf16),
        pltpu.VMEM((count, handlers, batch_rows, width), bf16),
        pltpu.VMEM((handlers, count, 1, batch_rows), i32),
        pltpu.VMEM((count, z_count, block, width), bf16),
        pltpu.VMEM((count, block, width), f32),
        pltpu.VMEM((count, z_count, block, width), bf16),
        pltpu.VMEM((count, handlers, rows_own, width), bf16),
        pltpu.VMEM((table_count, rows_own, width), bf16),
        pltpu.VMEM((handlers * z_count, rows_own, width), bf16),
        dma((7,)),
        dma((groups // (2 * UNROLL),)),
        dma,
        dma,
    ] + [dma((count,)) for _ in range(6)] + [dma, dma]
    results = pl.pallas_call(
        functools.partial(step_kernel, slots, direct, z_count, mp_count),
        out_shape=tuple(pltpu.VMEM(a.shape, a.dtype) for a in out_shape),
        in_specs=[hbm] * 8,
        out_specs=(vmem,) * 3,
        scratch_shapes=scratch,
        compiler_params=pltpu.CompilerParams(
            collective_id=0, has_side_effects=True, vmem_limit_bytes=VMEM_LIMIT
        ),
    )(
        sparse_vecs.transpose(1, 0, 2).reshape(table_count, groups, GROUP, width),
        dense_vec.reshape(groups, GROUP, width), top_cot, top_weight,
        owner_ids.transpose(1, 2, 0), local_rows.T, table, accum,
    )
    return pl.pallas_call(
        emit_kernel,
        out_shape=out_shape,
        in_specs=[vmem] * 3,
        out_specs=(any_spec,) * 3,
        scratch_shapes=[dma((3,))],
        compiler_params=pltpu.CompilerParams(vmem_limit_bytes=2 * 1024 * 1024),
    )(*results)


def solution(mesh):
    in_specs = (
        P(("dp", "mp"), None, None),
        P(("dp", "mp"), None),
        P(("dp", "mp"), None),
        P(),
        P(("dp", "mp"), None, None),
        P(("dp", "mp"), None),
        P(None, ("dp", "mp"), None),
        P(None, ("dp", "mp")),
    )
    out_specs = (P(("dp", "mp"), None), P(None, ("dp", "mp"), None), P(None, ("dp", "mp")))
    return jax.shard_map(
        per_device, mesh=mesh, in_specs=in_specs, out_specs=out_specs, check_vma=False
    )
```

```python
import functools

import jax
import jax.numpy as jnp
from jax import lax
from jax.experimental import pallas as pl
from jax.experimental.pallas import tpu as pltpu
from jax.sharding import PartitionSpec as P

LEARN_RATE = 0.1
EPSILON = 1e-08
MESH = pl.DeviceIdType.MESH
VMEM_LIMIT = 60 * 1024 * 1024
LANES = 128
GROUP = 8
SPAN = 256
UNROLL = 8
PARTS = (4, 10, 26)


def table_slots(table_count, handlers):
    slots = []
    rest = table_count % handlers
    counts = [handlers] * (table_count // handlers)
    if rest:
        counts.insert(min(1, len(counts)), rest)
    start = 0
    for count in counts:
        if count == handlers:
            slots.append((start, None))
        else:
            step = 2 if 2 * count <= handlers else 1
            owners = [i * (handlers - 2) // max(1, count - 1) for i in range(count)]
            slots.append((start, tuple(owners)))
        start += count
    return slots


def step_kernel(
    slots, direct, z_count, mp_count,
    sparse, dense, cot, weight, owner, local, table, accum,
    dense_out, table_out, accum_out,
    cot_v, weight_v, owner_v, local_v, table_v, accum_v,
    keys, pair_cot, select, repeat, blocks, spread, top, grads, got_rows, got_keys,
    partial, own_sum, z_in, fin_out, fin_in, pieces,
    load_sem, tile_sem, key_send, key_recv, row_send, row_recv,
    z_send, z_recv, fin_send, fin_recv, direct_send, direct_recv,
):
    table_count, groups, _, width = sparse.shape
    batch_rows = groups * GROUP
    rows_own = table.shape[1]
    handlers = 2 * mp_count
    rows_grp = rows_own * mp_count
    block = handlers * rows_own
    feature_count = table_count + 1
    dp, mp = lax.axis_index("dp"), lax.axis_index("mp")
    z, x = dp // 2, dp % 2
    me = x * mp_count + mp

    def plane_device(h):
        return (z * 2 + h // mp_count, h % mp_count)

    def z_device(d):
        return (((z + d) % z_count) * 2 + x, mp)

    def all_in(buffer, sem):
        pltpu.make_async_copy(buffer, buffer, sem).wait()

    loads = [
        pltpu.make_async_copy(source, target, load_sem.at[i])
        for i, (source, target) in enumerate((
            (cot, cot_v), (weight, weight_v), (owner, owner_v), (local, local_v),
            (dense, blocks.at[:, table_count]), (table, table_v), (accum, accum_v),
        ))
    ]
    tiles = [
        pltpu.make_async_copy(
            sparse.at[:, g], blocks.at[g, pl.ds(0, table_count)],
            tile_sem.at[g // (2 * UNROLL)],
        )
        for g in range(groups)
    ]
    for load in loads[:4]:
        load.start()
    blocks[:, pl.ds(feature_count, SPAN // GROUP - feature_count)] = jnp.zeros(
        (groups, SPAN // GROUP - feature_count, GROUP, width), jnp.bfloat16
    )

    barrier = pltpu.get_barrier_semaphore()
    device_count = 2 * z_count * mp_count

    def greet(step, carry):
        other = (dp * mp_count + mp + 1 + step) % device_count
        pl.semaphore_signal(
            barrier, inc=1, device_id=(other // mp_count, other % mp_count),
            device_id_type=MESH,
        )
        return carry

    lax.fori_loop(0, device_count - 1, greet, 0)

    with jax.named_scope("const"):
        pair_count = feature_count * (feature_count - 1) // 2
        feature_pad = SPAN // GROUP
        per_dot = LANES // feature_pad
        dots = -(-feature_count // per_dot)
        columns = lax.broadcasted_iota(jnp.int32, (1, dots * LANES), 1)
        left, right = columns // feature_pad, columns % feature_pad
        inside = (left < feature_count) & (right < feature_count) & (left != right)
        left = jnp.where(left == table_count, 0, left + 1)
        right = jnp.where(right == table_count, 0, right + 1)
        high, low = jnp.maximum(left, right), jnp.minimum(left, right)
        place = jnp.where(inside, high * (high - 1) // 2 + low, -1)
        pairs = lax.broadcasted_iota(jnp.int32, (pair_count, dots * LANES), 0)
        select[...] = jnp.where(pairs == place, 1.0, 0.0).astype(jnp.bfloat16)
        rep_row = lax.broadcasted_iota(jnp.int32, (LANES, per_dot * SPAN), 0)
        rep_col = lax.broadcasted_iota(jnp.int32, (LANES, per_dot * SPAN), 1)
        repeat[...] = jnp.where(rep_row == rep_col // GROUP, 1.0, 0.0).astype(jnp.bfloat16)
    with jax.named_scope("loadwait"):
        loads[0].wait()
        for load in loads[4:5] + tiles + loads[5:]:
            load.start()
        loads[1].wait()
    input_cot = lax.dot_general(
        cot_v[...], weight_v[...], (((1,), (1,)), ((), ())), preferred_element_type=jnp.float32
    )
    top[...] = input_cot[:, :width]
    pair_cot[...] = input_cot[:, width:].astype(jnp.bfloat16)

    with jax.named_scope("blocks"):
        loads[4].wait()

    features = blocks.reshape(groups, SPAN, width)
    mask = (
        lax.broadcasted_iota(jnp.int32, (GROUP, SPAN), 1) % GROUP
        == lax.broadcasted_iota(jnp.int32, (GROUP, SPAN), 0)
    )

    def gradients(first, last):
        for q in range(-(-first // per_dot), -(-last // per_dot)):
            symmetric = jnp.dot(
                pair_cot[...], select[:, q * LANES : (q + 1) * LANES],
                preferred_element_type=jnp.float32,
            ).astype(jnp.bfloat16)
            spread[:, q * per_dot * SPAN : (q + 1) * per_dot * SPAN] = jnp.dot(
                symmetric, repeat[...], preferred_element_type=jnp.float32
            )

        def one(step, carry):
            if first == 0:
                span = pl.ds(step * 2 * UNROLL, 2 * UNROLL)
                all_in(blocks.at[span, pl.ds(0, table_count)], tile_sem.at[step])
            for i in [step * UNROLL + u for u in range(UNROLL)]:
                outs = []
                for half in range(2):
                    rows = pl.ds(pl.multiple_of((2 * i + half) * GROUP, GROUP), GROUP)
                    parts = [
                        jnp.where(mask, spread[rows, t * SPAN : (t + 1) * SPAN], 0.0)
                        for t in range(first, last)
                    ]
                    lhs = jnp.concatenate(parts, 0).astype(jnp.bfloat16)
                    outs.append(
                        jnp.dot(lhs, features[2 * i + half], preferred_element_type=jnp.float32)
                    )
                span = pl.ds(pl.multiple_of(i * 2 * GROUP, 2 * GROUP), 2 * GROUP)
                for t in range(first, last):
                    at = (t - first) * GROUP
                    both = jnp.concatenate([out[at : at + GROUP] for out in outs], 0)
                    if t == table_count:
                        dense_out[span, :] = (both + top[span, :]).astype(jnp.bfloat16)
                    else:
                        grads[t, span, :] = both.astype(jnp.bfloat16)
            return carry

        lax.fori_loop(0, batch_rows // (2 * GROUP * UNROLL), one, 0)

    def table_of(slot, h):
        return slots[slot][0] + h // 2 + (h % 2) * (handlers // 2)

    def row_copy(slot, t, target, source):
        return pltpu.make_async_remote_copy(
            src_ref=grads.at[t],
            dst_ref=got_rows.at[slot, source],
            send_sem=row_send.at[slot],
            recv_sem=row_recv.at[slot],
            device_id=plane_device(target),
            device_id_type=MESH,
        )

    def key_copy(target, source):
        return pltpu.make_async_remote_copy(
            src_ref=keys.at[target],
            dst_ref=got_keys.at[source],
            send_sem=key_send,
            recv_sem=key_recv,
            device_id=plane_device(target),
            device_id_type=MESH,
        )

    def self_copy(slot, t):
        return pltpu.make_async_copy(grads.at[t], got_rows.at[slot, me], row_recv.at[slot])

    def targets_of(slot, parity):
        start, owners = slots[slot]
        if owners is None:
            rows_y = mp_count // 2
            hops = [(0, j) for j in range(1, rows_y)] + [(1, j) for j in range(rows_y)]
            for jx, jy in hops:
                h = 2 * ((x + jx) % 2 * rows_y + (mp // 2 + jy) % rows_y) + parity
                yield h, table_of(slot, h), None
            h = 2 * (me // 2) + parity
            yield h, table_of(slot, h), me != h
        else:
            for i, h in enumerate(owners):
                if h % 2 == parity:
                    yield h, start + i, me != h

    def guarded(condition, body):
        if condition is None:
            body()
        else:
            pl.when(condition)(body)

    def handled(slot, body, parity=None):
        start, owners = slots[slot]
        if owners is None:
            if parity is None:
                body(table_of(slot, me))
            else:
                guarded(me % 2 == parity, lambda: body(table_of(slot, me)))
        else:
            for i, h in enumerate(owners):
                if parity is None or h % 2 == parity:
                    guarded(me == h, lambda i=i: body(start + i))

    def send_rows(slot, parity):
        for h, t, condition in targets_of(slot, parity):
            guarded(condition, lambda: row_copy(slot, t, h, me).start())
        handled(slot, lambda t: self_copy(slot, t).start(), parity)

    def build_keys():
        for slot, (start, owners) in enumerate(slots):
            for h in range(handlers):
                if owners is None:
                    t = table_of(slot, h)
                else:
                    t = start + (owners.index(h) if h in owners else 0)
                keys[h, slot] = owner_v[t] * rows_grp + local_v[t : t + 1]
        for slot in range(len(slots)):
            got_keys[me, slot] = keys[me, slot]

    def send_keys():
        for d in range(1, handlers):
            key_copy((me + d) % handlers, me).start()

    def wait_sent(slot):
        start, owners = slots[slot]
        if owners is None:
            all_in(grads.at[pl.ds(0, handlers - 1)], row_send.at[slot])
        else:
            mine = [me == h for h in owners]
            mine = functools.reduce(jnp.logical_or, mine)
            for less in range(2):
                sent = len(owners) - less
                if sent:
                    guarded(
                        mine if less else jnp.logical_not(mine),
                        lambda: all_in(grads.at[pl.ds(0, sent)], row_send.at[slot]),
                    )

    def z_order(step):
        low = z_count - 1 - step
        low = low - jnp.where(low <= z, 1, 0)
        high = step + jnp.where(step >= z, 1, 0)
        return jnp.where(2 * z < z_count, low, high)

    def z_copy(slot, target, source):
        return pltpu.make_async_remote_copy(
            src_ref=partial.at[slot, target],
            dst_ref=z_in.at[slot, source],
            send_sem=z_send.at[slot],
            recv_sem=z_recv.at[slot],
            device_id=(target * 2 + x, mp),
            device_id_type=MESH,
        )

    def direct_copy(slot, target, h):
        return pltpu.make_async_remote_copy(
            src_ref=partial.at[slot, target, pl.ds(pl.multiple_of(h * rows_own, 16), rows_own)],
            dst_ref=pieces.at[me * z_count + z],
            send_sem=direct_send,
            recv_sem=direct_recv,
            device_id=(target * 2 + h // mp_count, h % mp_count),
            device_id_type=MESH,
        )

    def job(slot):
        def body(t):
            with jax.named_scope(f"jobwait{slot}"):
                all_in(got_rows.at[slot], row_recv.at[slot])
            targets = lax.broadcasted_iota(jnp.int32, (block, batch_rows), 0)

            def sums(target):
                base = target * block
                total = jnp.zeros((block, width), jnp.float32)
                for h in range(handlers):
                    onehot = jnp.where(targets == got_keys[h, slot] - base, 1.0, 0.0)
                    total = total + jnp.dot(
                        onehot.astype(jnp.bfloat16), got_rows[slot, h],
                        preferred_element_type=jnp.float32,
                    )
                return total

            def away(step, carry):
                target = z_order(step)
                partial[slot, target] = sums(target).astype(jnp.bfloat16)
                if slot == direct:
                    for h in range(handlers):
                        direct_copy(slot, target, h).start()
                else:
                    z_copy(slot, target, z).start()
                return carry

            lax.fori_loop(0, z_count - 1, away, 0)
            if slot == direct:
                partial[slot, z] = sums(z).astype(jnp.bfloat16)
                for d in range(1, handlers):
                    direct_copy(slot, z, (me + d) % handlers).start()
                span = pl.ds(pl.multiple_of(me * rows_own, 16), rows_own)
                pieces[me * z_count + z] = partial[slot, z, span]
            else:
                own_sum[slot] = sums(z)

        handled(slot, body)

    def fin_copy(slot, t, target, source):
        return pltpu.make_async_remote_copy(
            src_ref=fin_out.at[slot, target],
            dst_ref=fin_in.at[t],
            send_sem=fin_send.at[slot],
            recv_sem=fin_recv.at[slot],
            device_id=plane_device(target),
            device_id_type=MESH,
        )

    def finish(slot):
        def body(t):
            with jax.named_scope(f"finwait{slot}"):
                if z_count > 1:
                    all_in(z_in.at[slot, pl.ds(0, z_count - 1)], z_recv.at[slot])
            total = own_sum[slot]
            for d in range(1, z_count):
                total = total + z_in[slot, (z + d) % z_count].astype(jnp.float32)
            total = total.astype(jnp.bfloat16)
            for h in range(handlers):
                fin_out[slot, h] = total[h * rows_own : (h + 1) * rows_own]
            for d in range(1, handlers):
                fin_copy(slot, t, (me + d) % handlers, me).start()
            fin_in[t] = fin_out[slot, me]

        handled(slot, body)

    lane = lax.broadcasted_iota(jnp.int32, (rows_own, LANES), 1)
    state = {}

    def update(slot):
        start, owners = slots[slot]
        count = handlers if owners is None else len(owners)
        span = slice(start, start + count)
        if slot == direct:
            all_in(pieces.at[pl.ds(0, handlers * z_count - 1)], direct_recv)
            parts = [None] * handlers
            for h in range(handlers):
                total = pieces[h * z_count].astype(jnp.float32)
                for source in range(1, z_count):
                    total = total + pieces[h * z_count + source].astype(jnp.float32)
                parts[table_of(0, h) - slots[0][0]] = total
            grad = jnp.stack(parts)
        elif owners is None:
            all_in(fin_in.at[pl.ds(0, handlers - 1)], fin_recv.at[slot])
        else:
            mine = functools.reduce(jnp.logical_or, [me == h for h in owners])
            for less in range(2):
                came = count - less
                if came:
                    guarded(
                        mine if less else jnp.logical_not(mine),
                        lambda: all_in(fin_in.at[pl.ds(0, came)], fin_recv.at[slot]),
                    )
        if slot != direct:
            grad = fin_in[span].astype(jnp.float32)
        mean = jnp.sum(grad * grad, axis=2, keepdims=True) * (1.0 / width)
        old = jnp.stack([state["old"][:, t : t + 1] for t in range(start, start + count)])
        new = old + mean
        for i in range(count):
            state["new"] = jnp.where(lane == start + i, new[i], state["new"])
        table_out[span] = table_v[span] - grad * (LEARN_RATE / (jnp.sqrt(new) + EPSILON))

    def rows_of(slot):
        start, owners = slots[slot]
        return start, start + (handlers if owners is None else len(owners))

    count = len(slots)
    sends = []
    for slot in range(count):
        first, last = rows_of(slot)
        if slots[slot][1] is None:
            sends += [(slot, 0, first + handlers // 2), (slot, 1, last)]
        else:
            sends += [(slot, 0, last), (slot, 1, last)]
    done = 0
    for part, last in enumerate(PARTS):
        last = min(last, table_count)
        if part == len(PARTS) - 1:
            last = table_count
        with jax.named_scope(f"grad{part}"):
            gradients(done, last + (1 if last == table_count else 0))
        if part == 0:
            loads[2].wait()
            loads[3].wait()
            build_keys()
            with jax.named_scope("barrier"):
                pl.semaphore_wait(barrier, device_count - 1)
            send_keys()
        for slot, parity, ready in sends:
            if done < ready <= last or (parity and ready == last == table_count):
                send_rows(slot, parity)
        done = last

    loads[5].wait()
    loads[6].wait()
    old = jnp.concatenate(
        [accum_v[...], jnp.zeros((LANES - table_count, rows_own), jnp.float32)], 0
    )
    state["old"] = old.T
    state["new"] = jnp.zeros((rows_own, LANES), jnp.float32)

    all_in(got_keys.at[pl.ds(0, handlers - 1)], key_recv)

    plan = []
    for step in range(count + 1):
        plan += [(job, step)] * (step < count) + [(finish, step - 1)] * (step > 0)
    plan += [(update, slot) for slot in range(count)]
    plan = [(stage, slot) for stage, slot in plan if stage is not finish or slot != direct]
    for stage, slot in plan:
        with jax.named_scope(f"{stage.__name__}{slot}"):
            stage(slot)
    with jax.named_scope("accum"):
        accum_out[...] = state["new"].T[:table_count]

    all_in(keys.at[pl.ds(0, handlers - 1)], key_send)
    for slot in range(count):
      with jax.named_scope("sent"):
        wait_sent(slot)

        def sent(t):
            if slot == direct:
                all_in(pieces.at[pl.ds(0, handlers * z_count - 1)], direct_send)
                return
            if z_count > 1:
                all_in(partial.at[slot, pl.ds(0, z_count - 1)], z_send.at[slot])
            all_in(fin_out.at[slot, pl.ds(0, handlers - 1)], fin_send.at[slot])

        handled(slot, sent)


def emit_kernel(*refs):
    sources, targets, sem = refs[:3], refs[3:6], refs[6]
    copies = [
        pltpu.make_async_copy(source, target, sem.at[i])
        for i, (source, target) in enumerate(zip(sources, targets))
    ]
    for copy in copies:
        copy.start()
    for copy in copies:
        copy.wait()


def per_device(sparse_vecs, dense_vec, top_cot, top_weight, owner_ids, local_rows, table, accum):
    batch_rows, table_count, width = sparse_vecs.shape
    rows_own = table.shape[1]
    groups = batch_rows // GROUP
    z_count = lax.axis_size("dp") // 2
    mp_count = lax.axis_size("mp")
    handlers = 2 * mp_count
    slots = table_slots(table_count, handlers)
    count = len(slots)
    direct = count - 1 if slots[count - 1][1] is None else None
    block = handlers * rows_own
    feature_count = table_count + 1
    dots = -(-feature_count * (SPAN // GROUP) // LANES)
    any_spec = pl.BlockSpec(memory_space=pl.ANY)
    hbm = pl.BlockSpec(memory_space=pltpu.HBM)
    vmem = pl.BlockSpec(memory_space=pltpu.VMEM)
    dma = pltpu.SemaphoreType.DMA
    bf16, f32, i32 = jnp.bfloat16, jnp.float32, jnp.int32
    out_shape = (
        jax.ShapeDtypeStruct(dense_vec.shape, bf16),
        jax.ShapeDtypeStruct(table.shape, f32),
        jax.ShapeDtypeStruct(accum.shape, f32),
    )
    scratch = [
        pltpu.VMEM(top_cot.shape, bf16),
        pltpu.VMEM(top_weight.shape, bf16),
        pltpu.VMEM((table_count, 1, batch_rows), i32),
        pltpu.VMEM((table_count, batch_rows), i32),
        pltpu.VMEM(table.shape, f32),
        pltpu.VMEM(accum.shape, f32),
        pltpu.VMEM((handlers, count, 1, batch_rows), i32),
        pltpu.VMEM((batch_rows, feature_count * table_count // 2), bf16),
        pltpu.VMEM((feature_count * table_count // 2, dots * LANES), bf16),
        pltpu.VMEM((LANES, LANES // (SPAN // GROUP) * SPAN), bf16),
        pltpu.VMEM((groups, SPAN // GROUP, GROUP, width), bf16),
        pltpu.VMEM((batch_rows, dots * (LANES // (SPAN // GROUP)) * SPAN), f32),
        pltpu.VMEM((batch_rows, width), f32),
        pltpu.VMEM((table_count, batch_rows, width), bf16),
        pltpu.VMEM((count, handlers, batch_rows, width), bf16),
        pltpu.VMEM((handlers, count, 1, batch_rows), i32),
        pltpu.VMEM((count, z_count, block, width), bf16),
        pltpu.VMEM((count, block, width), f32),
        pltpu.VMEM((count, z_count, block, width), bf16),
        pltpu.VMEM((count, handlers, rows_own, width), bf16),
        pltpu.VMEM((table_count, rows_own, width), bf16),
        pltpu.VMEM((handlers * z_count, rows_own, width), bf16),
        dma((7,)),
        dma((groups // (2 * UNROLL),)),
        dma,
        dma,
    ] + [dma((count,)) for _ in range(6)] + [dma, dma]
    results = pl.pallas_call(
        functools.partial(step_kernel, slots, direct, z_count, mp_count),
        out_shape=tuple(pltpu.VMEM(a.shape, a.dtype) for a in out_shape),
        in_specs=[hbm] * 8,
        out_specs=(vmem,) * 3,
        scratch_shapes=scratch,
        compiler_params=pltpu.CompilerParams(
            collective_id=0, has_side_effects=True, vmem_limit_bytes=VMEM_LIMIT
        ),
    )(
        sparse_vecs.transpose(1, 0, 2).reshape(table_count, groups, GROUP, width),
        dense_vec.reshape(groups, GROUP, width), top_cot, top_weight,
        owner_ids.transpose(1, 2, 0), local_rows.T, table, accum,
    )
    return pl.pallas_call(
        emit_kernel,
        out_shape=out_shape,
        in_specs=[vmem] * 3,
        out_specs=(any_spec,) * 3,
        scratch_shapes=[dma((3,))],
        compiler_params=pltpu.CompilerParams(vmem_limit_bytes=2 * 1024 * 1024),
    )(*results)


def solution(mesh):
    in_specs = (
        P(("dp", "mp"), None, None),
        P(("dp", "mp"), None),
        P(("dp", "mp"), None),
        P(),
        P(("dp", "mp"), None, None),
        P(("dp", "mp"), None),
        P(None, ("dp", "mp"), None),
        P(None, ("dp", "mp")),
    )
    out_specs = (P(("dp", "mp"), None), P(None, ("dp", "mp"), None), P(None, ("dp", "mp")))
    return jax.shard_map(
        per_device, mesh=mesh, in_specs=in_specs, out_specs=out_specs, check_vma=False
    )
```

```python
import functools

import jax
import jax.numpy as jnp
from jax import lax
from jax.experimental import pallas as pl
from jax.experimental.pallas import tpu as pltpu
from jax.sharding import PartitionSpec as P

LEARN_RATE = 0.1
EPSILON = 1e-08
MESH = pl.DeviceIdType.MESH
VMEM_LIMIT = 60 * 1024 * 1024
LANES = 128
GROUP = 8
SPAN = 256
UNROLL = 8
PARTS = (4, 10, 18, 26)


def table_slots(table_count, handlers):
    slots = []
    rest = table_count % handlers
    counts = [handlers] * (table_count // handlers)
    if rest:
        counts.insert(min(1, len(counts)), rest)
    start = 0
    for count in counts:
        if count == handlers:
            slots.append((start, None))
        else:
            step = 2 if 2 * count <= handlers else 1
            owners = [i * (handlers - 2) // max(1, count - 1) for i in range(count)]
            slots.append((start, tuple(owners)))
        start += count
    return slots


def step_kernel(
    slots, direct, z_count, mp_count,
    sparse, dense, cot, weight, owner, local, table, accum,
    dense_out, table_out, accum_out,
    cot_v, weight_v, owner_v, local_v, table_v, accum_v,
    keys, pair_cot, select, repeat, blocks, spread, top, grads, got_rows, got_keys,
    partial, own_sum, z_in, fin_out, fin_in, pieces,
    load_sem, tile_sem, key_send, key_recv, row_send, row_recv,
    z_send, z_recv, fin_send, fin_recv, direct_send, direct_recv,
):
    table_count, groups, _, width = sparse.shape
    batch_rows = groups * GROUP
    rows_own = table.shape[1]
    handlers = 2 * mp_count
    rows_grp = rows_own * mp_count
    block = handlers * rows_own
    feature_count = table_count + 1
    dp, mp = lax.axis_index("dp"), lax.axis_index("mp")
    z, x = dp // 2, dp % 2
    me = x * mp_count + mp

    def plane_device(h):
        return (z * 2 + h // mp_count, h % mp_count)

    def z_device(d):
        return (((z + d) % z_count) * 2 + x, mp)

    def all_in(buffer, sem):
        pltpu.make_async_copy(buffer, buffer, sem).wait()

    loads = [
        pltpu.make_async_copy(source, target, load_sem.at[i])
        for i, (source, target) in enumerate((
            (cot, cot_v), (weight, weight_v), (owner, owner_v), (local, local_v),
            (dense, blocks.at[:, table_count]), (table, table_v), (accum, accum_v),
        ))
    ]
    tiles = [
        pltpu.make_async_copy(
            sparse.at[:, g], blocks.at[g, pl.ds(0, table_count)],
            tile_sem.at[g // (2 * UNROLL)],
        )
        for g in range(groups)
    ]
    for load in loads[:4]:
        load.start()
    blocks[:, pl.ds(feature_count, SPAN // GROUP - feature_count)] = jnp.zeros(
        (groups, SPAN // GROUP - feature_count, GROUP, width), jnp.bfloat16
    )

    barrier = pltpu.get_barrier_semaphore()
    device_count = 2 * z_count * mp_count

    def greet(step, carry):
        other = (dp * mp_count + mp + 1 + step) % device_count
        pl.semaphore_signal(
            barrier, inc=1, device_id=(other // mp_count, other % mp_count),
            device_id_type=MESH,
        )
        return carry

    lax.fori_loop(0, device_count - 1, greet, 0)

    with jax.named_scope("const"):
        pair_count = feature_count * (feature_count - 1) // 2
        feature_pad = SPAN // GROUP
        per_dot = LANES // feature_pad
        dots = -(-feature_count // per_dot)
        columns = lax.broadcasted_iota(jnp.int32, (1, dots * LANES), 1)
        left, right = columns // feature_pad, columns % feature_pad
        inside = (left < feature_count) & (right < feature_count) & (left != right)
        left = jnp.where(left == table_count, 0, left + 1)
        right = jnp.where(right == table_count, 0, right + 1)
        high, low = jnp.maximum(left, right), jnp.minimum(left, right)
        place = jnp.where(inside, high * (high - 1) // 2 + low, -1)
        pairs = lax.broadcasted_iota(jnp.int32, (pair_count, dots * LANES), 0)
        select[...] = jnp.where(pairs == place, 1.0, 0.0).astype(jnp.bfloat16)
        rep_row = lax.broadcasted_iota(jnp.int32, (LANES, per_dot * SPAN), 0)
        rep_col = lax.broadcasted_iota(jnp.int32, (LANES, per_dot * SPAN), 1)
        repeat[...] = jnp.where(rep_row == rep_col // GROUP, 1.0, 0.0).astype(jnp.bfloat16)
    with jax.named_scope("loadwait"):
        loads[0].wait()
        for load in loads[4:5] + tiles + loads[5:]:
            load.start()
        loads[1].wait()
    input_cot = lax.dot_general(
        cot_v[...], weight_v[...], (((1,), (1,)), ((), ())), preferred_element_type=jnp.float32
    )
    top[...] = input_cot[:, :width]
    pair_cot[...] = input_cot[:, width:].astype(jnp.bfloat16)

    with jax.named_scope("blocks"):
        loads[4].wait()

    features = blocks.reshape(groups, SPAN, width)
    mask = (
        lax.broadcasted_iota(jnp.int32, (GROUP, SPAN), 1) % GROUP
        == lax.broadcasted_iota(jnp.int32, (GROUP, SPAN), 0)
    )

    def gradients(first, last):
        for q in range(-(-first // per_dot), -(-last // per_dot)):
            symmetric = jnp.dot(
                pair_cot[...], select[:, q * LANES : (q + 1) * LANES],
                preferred_element_type=jnp.float32,
            ).astype(jnp.bfloat16)
            spread[:, q * per_dot * SPAN : (q + 1) * per_dot * SPAN] = jnp.dot(
                symmetric, repeat[...], preferred_element_type=jnp.float32
            )

        def one(step, carry):
            if first == 0:
                span = pl.ds(step * 2 * UNROLL, 2 * UNROLL)
                all_in(blocks.at[span, pl.ds(0, table_count)], tile_sem.at[step])
            for i in [step * UNROLL + u for u in range(UNROLL)]:
                outs = []
                for half in range(2):
                    rows = pl.ds(pl.multiple_of((2 * i + half) * GROUP, GROUP), GROUP)
                    parts = [
                        jnp.where(mask, spread[rows, t * SPAN : (t + 1) * SPAN], 0.0)
                        for t in range(first, last)
                    ]
                    lhs = jnp.concatenate(parts, 0).astype(jnp.bfloat16)
                    outs.append(
                        jnp.dot(lhs, features[2 * i + half], preferred_element_type=jnp.float32)
                    )
                span = pl.ds(pl.multiple_of(i * 2 * GROUP, 2 * GROUP), 2 * GROUP)
                for t in range(first, last):
                    at = (t - first) * GROUP
                    both = jnp.concatenate([out[at : at + GROUP] for out in outs], 0)
                    if t == table_count:
                        dense_out[span, :] = (both + top[span, :]).astype(jnp.bfloat16)
                    else:
                        grads[t, span, :] = both.astype(jnp.bfloat16)
            return carry

        lax.fori_loop(0, batch_rows // (2 * GROUP * UNROLL), one, 0)

    def table_of(slot, h):
        return slots[slot][0] + h // 2 + (h % 2) * (handlers // 2)

    def row_copy(slot, t, target, source):
        return pltpu.make_async_remote_copy(
            src_ref=grads.at[t],
            dst_ref=got_rows.at[slot, source],
            send_sem=row_send.at[slot],
            recv_sem=row_recv.at[slot],
            device_id=plane_device(target),
            device_id_type=MESH,
        )

    def key_copy(target, source):
        return pltpu.make_async_remote_copy(
            src_ref=keys.at[target],
            dst_ref=got_keys.at[source],
            send_sem=key_send,
            recv_sem=key_recv,
            device_id=plane_device(target),
            device_id_type=MESH,
        )

    def self_copy(slot, t):
        return pltpu.make_async_copy(grads.at[t], got_rows.at[slot, me], row_recv.at[slot])

    def targets_of(slot, parity):
        start, owners = slots[slot]
        if owners is None:
            rows_y = mp_count // 2
            hops = [(0, j) for j in range(1, rows_y)] + [(1, j) for j in range(rows_y)]
            for jx, jy in hops:
                h = 2 * ((x + jx) % 2 * rows_y + (mp // 2 + jy) % rows_y) + parity
                yield h, table_of(slot, h), None
            h = 2 * (me // 2) + parity
            yield h, table_of(slot, h), me != h
        else:
            for i, h in enumerate(owners):
                if h % 2 == parity:
                    yield h, start + i, me != h

    def guarded(condition, body):
        if condition is None:
            body()
        else:
            pl.when(condition)(body)

    def handled(slot, body, parity=None):
        start, owners = slots[slot]
        if owners is None:
            if parity is None:
                body(table_of(slot, me))
            else:
                guarded(me % 2 == parity, lambda: body(table_of(slot, me)))
        else:
            for i, h in enumerate(owners):
                if parity is None or h % 2 == parity:
                    guarded(me == h, lambda i=i: body(start + i))

    def send_rows(slot, parity):
        for h, t, condition in targets_of(slot, parity):
            guarded(condition, lambda: row_copy(slot, t, h, me).start())
        handled(slot, lambda t: self_copy(slot, t).start(), parity)

    def build_keys():
        for slot, (start, owners) in enumerate(slots):
            for h in range(handlers):
                if owners is None:
                    t = table_of(slot, h)
                else:
                    t = start + (owners.index(h) if h in owners else 0)
                keys[h, slot] = owner_v[t] * rows_grp + local_v[t : t + 1]
        for slot in range(len(slots)):
            got_keys[me, slot] = keys[me, slot]

    def send_keys():
        for d in range(1, handlers):
            key_copy((me + d) % handlers, me).start()

    def wait_sent(slot):
        start, owners = slots[slot]
        if owners is None:
            all_in(grads.at[pl.ds(0, handlers - 1)], row_send.at[slot])
        else:
            mine = [me == h for h in owners]
            mine = functools.reduce(jnp.logical_or, mine)
            for less in range(2):
                sent = len(owners) - less
                if sent:
                    guarded(
                        mine if less else jnp.logical_not(mine),
                        lambda: all_in(grads.at[pl.ds(0, sent)], row_send.at[slot]),
                    )

    def z_order(step):
        low = z_count - 1 - step
        low = low - jnp.where(low <= z, 1, 0)
        high = step + jnp.where(step >= z, 1, 0)
        return jnp.where(2 * z < z_count, low, high)

    def z_copy(slot, target, source):
        return pltpu.make_async_remote_copy(
            src_ref=partial.at[slot, target],
            dst_ref=z_in.at[slot, source],
            send_sem=z_send.at[slot],
            recv_sem=z_recv.at[slot],
            device_id=(target * 2 + x, mp),
            device_id_type=MESH,
        )

    def direct_copy(slot, target, h):
        return pltpu.make_async_remote_copy(
            src_ref=partial.at[slot, target, pl.ds(pl.multiple_of(h * rows_own, 16), rows_own)],
            dst_ref=pieces.at[me * z_count + z],
            send_sem=direct_send,
            recv_sem=direct_recv,
            device_id=(target * 2 + h // mp_count, h % mp_count),
            device_id_type=MESH,
        )

    def job(slot):
        def body(t):
            with jax.named_scope(f"jobwait{slot}"):
                all_in(got_rows.at[slot], row_recv.at[slot])
            targets = lax.broadcasted_iota(jnp.int32, (block, batch_rows), 0)

            def sums(target):
                base = target * block
                total = None
                for h in range(handlers):
                    onehot = jnp.where(targets == got_keys[h, slot] - base, 1.0, 0.0)
                    part = jnp.dot(
                        onehot.astype(jnp.bfloat16), got_rows[slot, h],
                        preferred_element_type=jnp.float32,
                    )
                    total = part if total is None else total + part
                return total

            def away(step, carry):
                target = z_order(step)
                partial[slot, target] = sums(target).astype(jnp.bfloat16)
                if slot == direct:
                    for h in range(handlers):
                        direct_copy(slot, target, h).start()
                else:
                    z_copy(slot, target, z).start()
                return carry

            lax.fori_loop(0, z_count - 1, away, 0)
            if slot == direct:
                partial[slot, z] = sums(z).astype(jnp.bfloat16)
                for d in range(1, handlers):
                    direct_copy(slot, z, (me + d) % handlers).start()
                span = pl.ds(pl.multiple_of(me * rows_own, 16), rows_own)
                pieces[me * z_count + z] = partial[slot, z, span]
            else:
                own_sum[slot] = sums(z)

        handled(slot, body)

    def fin_copy(slot, t, target, source):
        return pltpu.make_async_remote_copy(
            src_ref=fin_out.at[slot, target],
            dst_ref=fin_in.at[t],
            send_sem=fin_send.at[slot],
            recv_sem=fin_recv.at[slot],
            device_id=plane_device(target),
            device_id_type=MESH,
        )

    def finish(slot):
        def body(t):
            with jax.named_scope(f"finwait{slot}"):
                if z_count > 1:
                    all_in(z_in.at[slot, pl.ds(0, z_count - 1)], z_recv.at[slot])
            total = own_sum[slot]
            for d in range(1, z_count):
                total = total + z_in[slot, (z + d) % z_count].astype(jnp.float32)
            total = total.astype(jnp.bfloat16)
            for h in range(handlers):
                fin_out[slot, h] = total[h * rows_own : (h + 1) * rows_own]
            for d in range(1, handlers):
                fin_copy(slot, t, (me + d) % handlers, me).start()
            fin_in[t] = fin_out[slot, me]

        handled(slot, body)

    lane = lax.broadcasted_iota(jnp.int32, (rows_own, LANES), 1)
    state = {}

    def update(slot):
        start, owners = slots[slot]
        count = handlers if owners is None else len(owners)
        span = slice(start, start + count)
        if slot == direct:
            all_in(pieces.at[pl.ds(0, handlers * z_count - 1)], direct_recv)
            parts = [None] * handlers
            for h in range(handlers):
                total = pieces[h * z_count].astype(jnp.float32)
                for source in range(1, z_count):
                    total = total + pieces[h * z_count + source].astype(jnp.float32)
                parts[table_of(0, h) - slots[0][0]] = total
            grad = jnp.stack(parts)
        elif owners is None:
            all_in(fin_in.at[pl.ds(0, handlers - 1)], fin_recv.at[slot])
        else:
            mine = functools.reduce(jnp.logical_or, [me == h for h in owners])
            for less in range(2):
                came = count - less
                if came:
                    guarded(
                        mine if less else jnp.logical_not(mine),
                        lambda: all_in(fin_in.at[pl.ds(0, came)], fin_recv.at[slot]),
                    )
        if slot != direct:
            grad = fin_in[span].astype(jnp.float32)
        mean = jnp.sum(grad * grad, axis=2, keepdims=True) * (1.0 / width)
        old = jnp.stack([state["old"][:, t : t + 1] for t in range(start, start + count)])
        new = old + mean
        for i in range(count):
            state["new"] = jnp.where(lane == start + i, new[i], state["new"])
        table_out[span] = table_v[span] - grad * (LEARN_RATE / (jnp.sqrt(new) + EPSILON))

    def rows_of(slot):
        start, owners = slots[slot]
        return start, start + (handlers if owners is None else len(owners))

    count = len(slots)
    sends = []
    for slot in range(count):
        first, last = rows_of(slot)
        if slots[slot][1] is None:
            sends += [(slot, 0, first + handlers // 2), (slot, 1, last)]
        else:
            sends += [(slot, 0, last), (slot, 1, last)]
    done = 0
    for part, last in enumerate(PARTS):
        last = min(last, table_count)
        if part == len(PARTS) - 1:
            last = table_count
        with jax.named_scope(f"grad{part}"):
            gradients(done, last + (1 if last == table_count else 0))
        if part == 0:
            loads[2].wait()
            loads[3].wait()
            build_keys()
            with jax.named_scope("barrier"):
                pl.semaphore_wait(barrier, device_count - 1)
            send_keys()
        for slot, parity, ready in sends:
            if done < ready <= last or (parity and ready == last == table_count):
                send_rows(slot, parity)
        done = last

    loads[5].wait()
    loads[6].wait()
    old = jnp.concatenate(
        [accum_v[...], jnp.zeros((LANES - table_count, rows_own), jnp.float32)], 0
    )
    state["old"] = old.T
    state["new"] = jnp.zeros((rows_own, LANES), jnp.float32)

    all_in(got_keys.at[pl.ds(0, handlers - 1)], key_recv)

    plan = []
    for step in range(count + 1):
        plan += [(job, step)] * (step < count) + [(finish, step - 1)] * (step > 0)
    plan += [(update, slot) for slot in range(count)]
    plan = [(stage, slot) for stage, slot in plan if stage is not finish or slot != direct]
    for stage, slot in plan:
        with jax.named_scope(f"{stage.__name__}{slot}"):
            stage(slot)
    with jax.named_scope("accum"):
        accum_out[...] = state["new"].T[:table_count]

    all_in(keys.at[pl.ds(0, handlers - 1)], key_send)
    for slot in range(count):
      with jax.named_scope("sent"):
        wait_sent(slot)

        def sent(t):
            if slot == direct:
                all_in(pieces.at[pl.ds(0, handlers * z_count - 1)], direct_send)
                return
            if z_count > 1:
                all_in(partial.at[slot, pl.ds(0, z_count - 1)], z_send.at[slot])
            all_in(fin_out.at[slot, pl.ds(0, handlers - 1)], fin_send.at[slot])

        handled(slot, sent)


def emit_kernel(*refs):
    sources, targets, sem = refs[:3], refs[3:6], refs[6]
    copies = [
        pltpu.make_async_copy(source, target, sem.at[i])
        for i, (source, target) in enumerate(zip(sources, targets))
    ]
    for copy in copies:
        copy.start()
    for copy in copies:
        copy.wait()


def per_device(sparse_vecs, dense_vec, top_cot, top_weight, owner_ids, local_rows, table, accum):
    batch_rows, table_count, width = sparse_vecs.shape
    rows_own = table.shape[1]
    groups = batch_rows // GROUP
    z_count = lax.axis_size("dp") // 2
    mp_count = lax.axis_size("mp")
    handlers = 2 * mp_count
    slots = table_slots(table_count, handlers)
    count = len(slots)
    direct = count - 1 if slots[count - 1][1] is None else None
    block = handlers * rows_own
    feature_count = table_count + 1
    dots = -(-feature_count * (SPAN // GROUP) // LANES)
    any_spec = pl.BlockSpec(memory_space=pl.ANY)
    hbm = pl.BlockSpec(memory_space=pltpu.HBM)
    vmem = pl.BlockSpec(memory_space=pltpu.VMEM)
    dma = pltpu.SemaphoreType.DMA
    bf16, f32, i32 = jnp.bfloat16, jnp.float32, jnp.int32
    out_shape = (
        jax.ShapeDtypeStruct(dense_vec.shape, bf16),
        jax.ShapeDtypeStruct(table.shape, f32),
        jax.ShapeDtypeStruct(accum.shape, f32),
    )
    scratch = [
        pltpu.VMEM(top_cot.shape, bf16),
        pltpu.VMEM(top_weight.shape, bf16),
        pltpu.VMEM((table_count, 1, batch_rows), i32),
        pltpu.VMEM((table_count, batch_rows), i32),
        pltpu.VMEM(table.shape, f32),
        pltpu.VMEM(accum.shape, f32),
        pltpu.VMEM((handlers, count, 1, batch_rows), i32),
        pltpu.VMEM((batch_rows, feature_count * table_count // 2), bf16),
        pltpu.VMEM((feature_count * table_count // 2, dots * LANES), bf16),
        pltpu.VMEM((LANES, LANES // (SPAN // GROUP) * SPAN), bf16),
        pltpu.VMEM((groups, SPAN // GROUP, GROUP, width), bf16),
        pltpu.VMEM((batch_rows, dots * (LANES // (SPAN // GROUP)) * SPAN), f32),
        pltpu.VMEM((batch_rows, width), f32),
        pltpu.VMEM((table_count, batch_rows, width), bf16),
        pltpu.VMEM((count, handlers, batch_rows, width), bf16),
        pltpu.VMEM((handlers, count, 1, batch_rows), i32),
        pltpu.VMEM((count, z_count, block, width), bf16),
        pltpu.VMEM((count, block, width), f32),
        pltpu.VMEM((count, z_count, block, width), bf16),
        pltpu.VMEM((count, handlers, rows_own, width), bf16),
        pltpu.VMEM((table_count, rows_own, width), bf16),
        pltpu.VMEM((handlers * z_count, rows_own, width), bf16),
        dma((7,)),
        dma((groups // (2 * UNROLL),)),
        dma,
        dma,
    ] + [dma((count,)) for _ in range(6)] + [dma, dma]
    results = pl.pallas_call(
        functools.partial(step_kernel, slots, direct, z_count, mp_count),
        out_shape=tuple(pltpu.VMEM(a.shape, a.dtype) for a in out_shape),
        in_specs=[hbm] * 8,
        out_specs=(vmem,) * 3,
        scratch_shapes=scratch,
        compiler_params=pltpu.CompilerParams(
            collective_id=0, has_side_effects=True, vmem_limit_bytes=VMEM_LIMIT
        ),
    )(
        sparse_vecs.transpose(1, 0, 2).reshape(table_count, groups, GROUP, width),
        dense_vec.reshape(groups, GROUP, width), top_cot, top_weight,
        owner_ids.transpose(1, 2, 0), local_rows.T, table, accum,
    )
    return pl.pallas_call(
        emit_kernel,
        out_shape=out_shape,
        in_specs=[vmem] * 3,
        out_specs=(any_spec,) * 3,
        scratch_shapes=[dma((3,))],
        compiler_params=pltpu.CompilerParams(vmem_limit_bytes=2 * 1024 * 1024),
    )(*results)


def solution(mesh):
    in_specs = (
        P(("dp", "mp"), None, None),
        P(("dp", "mp"), None),
        P(("dp", "mp"), None),
        P(),
        P(("dp", "mp"), None, None),
        P(("dp", "mp"), None),
        P(None, ("dp", "mp"), None),
        P(None, ("dp", "mp")),
    )
    out_specs = (P(("dp", "mp"), None), P(None, ("dp", "mp"), None), P(None, ("dp", "mp")))
    return jax.shard_map(
        per_device, mesh=mesh, in_specs=in_specs, out_specs=out_specs, check_vma=False
    )
```
